32 devices in a mesh: shift: 2 (over y), expert: 4 (over z), shard: 4 (over x, core).
Axes of the slice: x: 2, y: 2, z: 4, core: 2. Of those that a mesh axis runs over, the one named last changes fastest.
Arguments:
- master_gate: float32 [128, 2048, 1024], P(('shift', 'expert'), 'shard'), parts along dimension 0, may hold values from -0.1875 to 0.1875
- master_up: float32 [128, 2048, 1024], P(('shift', 'expert'), 'shard'), parts along dimension 0, may hold values from -0.1875 to 0.1875
- router_weight: float32 [4096, 64], P(('shift', 'shard'), 'expert'), parts along dimension 0, may hold values from -0.125 to 0.125
- router_gain: float32 [4096], P(('shift', 'shard')), parts along dimension 0, may hold values from 0.25 to 1.75
Outputs:
- final_gate: bfloat16 [128, 2048, 1024], P(('shift', 'expert'), None, 'shard'), parts along dimension 0
- final_up: bfloat16 [128, 2048, 1024], P(('shift', 'expert'), None, 'shard'), parts along dimension 0
- scale_gate: float32 [128, 1024], P(('shift', 'expert'), 'shard'), parts along dimension 0
- scale_up: float32 [128, 1024], P(('shift', 'expert'), 'shard'), parts along dimension 0
- serve_router: bfloat16 [4096, 64], P('shift'), parts along dimension 0
The draws below stay inside these ranges and needn't reach their ends.
There are 2 independent parts, one for each index of `shift`. The reference program is written for one: setup_inputs(seed, part) draws one part's arguments, and reference() takes and returns one part's arrays. A program takes and returns all parts, laid end to end along the dimension named above; each array names one. Nothing has to cross between parts.
All inputs are finite; a program needn't handle non-finite values. Where the reference program divides by a largest or mean magnitude, that divisor is 1e-20 or more.
Results may differ from the reference program's by a relative error of at most 0.001.
Values may be sent and summed in bfloat16 or wider, within the bound.
A program may use at most 256 MiB of HBM per device.

```python
import jax
import jax.numpy as jnp

EXPERTS = 64
D_MODEL = 2048
D_EXPERT = 1024


def spiked(values, rng, source, target, blocks, factor):
    def block_of(axis_at):
        return (jnp.arange(values.shape[axis_at]) // (values.shape[axis_at] // blocks)).reshape((-1,) + (1,) * (values.ndim - 1 - axis_at))

    first = jax.random.permutation(rng, blocks)[block_of(target)]
    second = (block_of(target) + blocks // 2) % blocks
    return jnp.where((block_of(source) == first) | (block_of(source) == second), factor * values, values)


def block_levels(stream_key, shape, split, smallest, high):
    gain = 1.0
    for dim, shards_of in split:
        steps = jax.random.uniform(jax.random.fold_in(jax.random.fold_in(stream_key, 6), dim), (shards_of,), jnp.float32, smallest / len(split), high / len(split))
        gain = gain * jnp.repeat(jnp.exp(steps), shape[dim] // shards_of).reshape((-1,) + (1,) * (len(shape) - 1 - dim))
    return gain


def bell_draw(rng, shape, width, reach, cuts=(), held_as=jnp.bfloat16):
    values = jax.random.normal(rng, shape, jnp.float32) * width
    if len(cuts) > 0:
        values = block_levels(rng, shape, cuts, -0.22, 0.18) * values
    return jnp.clip(values, min=-reach, max=reach).astype(held_as)


def bell_draw_with(stream_key, dims, spread, most, pieces, heavy, kind=jnp.bfloat16):
    array = spread * jax.random.normal(stream_key, dims, jnp.float32)
    if pieces:
        array = array * block_levels(stream_key, dims, pieces, -0.22, 0.18)
    return jnp.clip(spiked(array, jax.random.fold_in(stream_key, 3), *heavy), -most, most).astype(kind)


def setup_inputs(seed: int = 0, part: int = 0) -> dict:
    seeds = jax.random.split(jax.random.key(seed), 5)
    part_splits = jax.random.split(jax.random.fold_in(seeds[4], part), 5)
    master_gate = bell_draw_with(part_splits[0], (EXPERTS, D_MODEL, D_EXPERT), D_MODEL ** -0.5, 0.1875, ((0, 4), (1, 4)), (1, 2, 4, 2.0), jnp.float32)
    master_up = bell_draw_with(part_splits[1], (EXPERTS, D_MODEL, D_EXPERT), D_MODEL ** -0.5, 0.1875, ((0, 4), (1, 4)), (1, 2, 4, 2.0), jnp.float32)
    router_weight = bell_draw(part_splits[2], (D_MODEL, EXPERTS), D_MODEL ** -0.5, 0.125, ((0, 4), (1, 4)), jnp.float32)
    router_gain = jnp.clip(1.0 + 0.15 * jax.random.normal(part_splits[3], (D_MODEL,), jnp.float32), 0.25, 1.75)
    return dict(master_gate=master_gate, master_up=master_up, router_weight=router_weight, router_gain=router_gain)


def reference(master_gate, master_up, router_weight, router_gain):
    scale_gate = jnp.max(jnp.abs(master_gate), axis=1)
    final_gate = (master_gate / jnp.expand_dims(scale_gate, 1)).astype(jnp.bfloat16)
    scale_up = jnp.max(jnp.abs(master_up), axis=1)
    final_up = (master_up / jnp.expand_dims(scale_up, 1)).astype(jnp.bfloat16)
    serve_router = (router_weight * router_gain[:, None]).astype(jnp.bfloat16)
    return final_gate, final_up, scale_gate, scale_up, serve_router
```

```python
import functools

import jax
import jax.numpy as jnp
from jax import lax
from jax.experimental import pallas as pl
from jax.experimental.pallas import tpu as pltpu
from jax.sharding import PartitionSpec as P

MESH = pl.DeviceIdType.MESH
LANES = 128
TAIL = 2
RAMP = 3
AHEAD = 3
SLOTS = 5


def shift(shard, d, f, chips):
    return 2 * ((shard // 2 + d) % chips) + (shard % 2 + f) % 2


def exchange(n, groups, gate, up, router, gain, *refs):
    chips = n // 2
    away = [(d, f) for d in range(1, chips) for f in (0, 1)]
    narrow, near, *far = refs[: 2 + len(away)]
    (
        scale_gate, scale_up, routers, held, out, part, passed, mine, beside, whole, cross, full,
        direct, load_sem, near_send, near_recv, cross_send, cross_recv, full_send, full_recv,
        direct_send, direct_recv, send_sem, recv_sem, keep_sem, tail_recv, pass_send, pass_recv,
        rt_send, rt_recv, rt_keep,
    ) = refs[2 + len(away) :]
    me, group = lax.axis_index("shard"), lax.axis_index("expert")
    core = lax.rem(me, 2)
    items, rows, width, depth = 2 * gate.shape[0], gate.shape[1], out.shape[3], held.shape[0]
    blocks, per, half = gate.shape[2] // LANES, width // LANES, gate.shape[2] // LANES // 2
    share, tokens = part.shape
    last = items - near.shape[0]
    column = [(f, g) for g in range(groups) for f in (0, 1) if (f, g) != (0, 0)]

    def peer(d, f):
        return 2 * lax.rem(me // 2 + d, chips) + lax.rem(core + f, 2)

    def device(d, f, g=0):
        return {"shard": peer(d, f), "expert": lax.rem(group + g, groups)}

    def remote(src, dst, send, recv, to):
        return pltpu.make_async_remote_copy(
            src, dst, send, recv, device_id=to, device_id_type=MESH
        )

    def await_bytes(ref, sem):
        pltpu.make_async_copy(ref, ref, sem).wait()

    def load(k):
        slot, expert = lax.rem(k, depth), k // 2

        @pl.when(lax.rem(k, 2) == 0)
        def _():
            pltpu.make_async_copy(gate.at[expert], held.at[slot], load_sem.at[slot]).start()

        @pl.when(lax.rem(k, 2) == 1)
        def _():
            pltpu.make_async_copy(up.at[expert], held.at[slot], load_sem.at[slot]).start()

    def local(k):
        slot = lax.rem(k, depth)
        await_bytes(held.at[slot], load_sem.at[slot])
        for b in range(blocks):
            values = held[slot, :, b * LANES : (b + 1) * LANES]
            mine[k, b // half, b % half : b % half + 1, :] = jnp.max(
                jnp.abs(values), axis=0, keepdims=True
            )

    def tell(k):
        remote(mine.at[k], beside.at[k], near_send, near_recv.at[k], device(0, 1)).start()

    def ask(k):
        await_bytes(beside.at[k], near_recv.at[k])
        whole[k] = jnp.maximum(mine[k], beside[k])
        for d in range(1, chips):
            remote(
                whole.at[k, core], cross.at[k, d - 1], cross_send, cross_recv.at[k], device(d, 0)
            ).start()

    def relay(k):
        await_bytes(cross.at[k], cross_recv.at[k])
        most = whole[k, core]
        for d in range(1, chips):
            most = jnp.maximum(most, cross[k, d - 1])
        full[k, core] = most
        remote(full.at[k, core], full.at[k, core], full_send, full_recv.at[k], device(0, 1)).start()

    def place(k):
        return narrow.at[lax.rem(k, 2), k // 2, pl.ds(pl.multiple_of(me * rows, rows), rows)]

    def send(k):
        slot = lax.rem(k, SLOTS)
        for d, f in away + [(0, 1)]:
            remote(
                out.at[slot, peer(d, f)], place(k), send_sem.at[slot],
                recv_sem.at[2 * d + f - 1], device(d, f),
            ).start()
        pltpu.make_async_copy(out.at[slot, me], place(k), keep_sem.at[slot]).start()

    def sent(k):
        slot = lax.rem(k, SLOTS)
        await_bytes(out.at[slot, pl.ds(0, n - 1)], send_sem.at[slot])
        await_bytes(out.at[slot, 0], keep_sem.at[slot])

    def leave(k):
        slot, i = lax.rem(k, SLOTS), k - last
        remote(
            out.at[slot, peer(0, 1)], near.at[i, core], send_sem.at[slot], tail_recv, device(0, 1)
        ).start()
        pltpu.make_async_copy(out.at[slot, me], near.at[i, core], keep_sem.at[slot]).start()
        for (d, f), ref in zip(away, far):
            pltpu.make_async_copy(out.at[slot, peer(d, f)], ref.at[i], keep_sem.at[slot]).start()

    def left(k):
        slot = lax.rem(k, SLOTS)
        await_bytes(out.at[slot, 0], send_sem.at[slot])
        await_bytes(out.at[slot, pl.ds(0, n - 1)], keep_sem.at[slot])

    def home(shard):
        return routers.at[
            pl.ds(pl.multiple_of(group * share, share), share),
            pl.ds(pl.multiple_of(shard * tokens, tokens), tokens),
        ]

    def spread_router(block, shard):
        for i, (f, g) in enumerate(column):
            remote(block, home(shard), rt_send.at[i], rt_recv.at[i], device(0, f, g)).start()
        pltpu.make_async_copy(block, home(shard), rt_keep).start()

    for k in range(AHEAD):
        load(jnp.int32(k))
    barrier = pltpu.get_barrier_semaphore()
    for to in [device(d, f) for d, f in away] + [device(0, f, g) for f, g in column]:
        pl.semaphore_signal(barrier, inc=1, device_id=to, device_id_type=MESH)
    part[...] = (router[...] * gain[...]).astype(jnp.bfloat16)
    local(0)
    load(jnp.int32(AHEAD))
    pl.semaphore_wait(barrier, len(away) + len(column))
    for j, (d, f) in enumerate(away + [(0, 1)]):
        remote(mine.at[0], direct.at[j], direct_send, direct_recv, device(d, f)).start()
    for d in range(1, chips):
        remote(part, passed.at[d - 1], pass_send, pass_recv, device(d, 0)).start()
    spread_router(part, me)
    local(1)
    load(jnp.int32(AHEAD + 1))
    tell(1)
    ask(1)
    await_bytes(direct, direct_recv)
    most = mine[0]
    for j in range(n - 1):
        most = jnp.maximum(most, direct[j])
    full[0] = most

    def step(q, _):
        @pl.when(q > 0)
        def _():
            await_bytes(full.at[q, 0], full_recv.at[q])

        @pl.when(q >= SLOTS)
        def _():
            sent(q - SLOTS)

        slot, source = lax.rem(q, SLOTS), lax.rem(q, depth)
        for b in range(blocks):
            at = (b % per) * LANES
            values = held[source, :, b * LANES : (b + 1) * LANES]
            scale = full[q, b // half, b % half : b % half + 1, :]
            out[slot, b // per, :, at : at + LANES] = (values / scale).astype(jnp.bfloat16)

        @pl.when(q < last)
        def _():
            send(q)

        @pl.when(q >= last)
        def _():
            leave(q)

        first = q + jnp.minimum(q, RAMP) + 2
        leads = [(first, first < items), (first + 1, q < RAMP)]
        for k, due in leads:
            @pl.when(due)
            def _():
                local(k)
                tell(k)

                @pl.when(k + AHEAD < items)
                def _():
                    load(k + AHEAD)

        for k, due in leads:
            @pl.when(due)
            def _():
                ask(k)

        @pl.when(q + 1 < items)
        def _():
            relay(q + 1)

        @pl.when(q == RAMP)
        def _():
            await_bytes(passed, pass_recv)
            for d in range(1, chips):
                spread_router(passed.at[d - 1], peer(chips - d, 0))

        return 0

    lax.fori_loop(0, items, step, 0)

    for e in range(items // 2):
        for which, ref in enumerate((scale_gate, scale_up)):
            for i in range(per):
                b = me * per + i
                ref[e : e + 1, i * LANES : (i + 1) * LANES] = full[
                    2 * e + which, b // half, pl.ds(lax.rem(b, half), 1), :
                ]

    def drain(k, _):
        sent(k)
        return 0

    lax.fori_loop(items - SLOTS, last, drain, 0)

    def drain_tail(k, _):
        left(k)
        return 0

    lax.fori_loop(last, items, drain_tail, 0)
    await_bytes(beside.at[pl.ds(1, items - 1)], near_send)
    await_bytes(cross.at[pl.ds(1, items - 1)], cross_send)
    await_bytes(full.at[pl.ds(1, items - 1), 0], full_send)
    await_bytes(direct, direct_send)
    await_bytes(passed, pass_send)
    strip = routers.at[pl.ds(0, share), pl.ds(0, chips * tokens)]
    for i in range(len(column)):
        await_bytes(strip, rt_send.at[i])
        await_bytes(strip, rt_recv.at[i])
    await_bytes(strip, rt_keep)
    await_bytes(near.at[:, 0], tail_recv)
    for j in range(n - 1):
        await_bytes(narrow.at[:, :, pl.ds(0, rows)], recv_sem.at[j])


def spread(narrow, gate, up):
    gate[...] = narrow[0]
    up[...] = narrow[1]


def finish(n, pieces, extras, *refs):
    count = len(pieces)
    arrived, small, results, sems = (
        refs[:count], refs[count : count + extras], refs[count + extras + 2 : -1], refs[-1]
    )
    gate, up, *copies = results
    me, chips = lax.axis_index("shard"), n // 2
    experts, tail, rows = gate.shape[0], arrived[0].shape[0], gate.shape[1] // n
    for at, (piece, ref) in enumerate(zip(pieces, arrived)):
        for i in range(tail):
            final = (gate, up)[i % 2].at[experts - tail // 2 + i // 2]
            for c in range(ref.shape[1]):
                if piece is None:
                    source = 2 * (me // 2) + c
                else:
                    d, f = piece
                    source = 2 * lax.rem(me // 2 + chips - d, chips) + lax.rem(me % 2 + f, 2)
                to = final.at[pl.ds(pl.multiple_of(source * rows, rows), rows)]
                pltpu.make_async_copy(ref.at[i, c], to, sems.at[at]).start()
    for ref, copy in zip(small, copies):
        copy[...] = ref[...]
    for at, ref in enumerate(arrived):
        pltpu.make_async_copy(ref, ref, sems.at[at]).wait()


def by_kernel(n, groups, gate, up, router, gain):
    experts, rows, columns = gate.shape
    width, items, depth, chips = columns // n, 2 * experts, RAMP + AHEAD + 2, n // 2
    tokens, share = router.shape
    half = columns // LANES // 2
    away = [(d, f) for d in range(1, chips) for f in (0, 1)]
    column = 2 * groups - 1
    anywhere = pl.BlockSpec(memory_space=pl.ANY)
    inside = pl.BlockSpec(memory_space=pltpu.VMEM)
    dma = pltpu.SemaphoreType.DMA
    bf16 = functools.partial(jax.ShapeDtypeStruct, dtype=jnp.bfloat16)
    maxima = pltpu.VMEM((items, 2, half, LANES), jnp.float32)
    narrow, near, *far, scale_gate, scale_up, routers = pl.pallas_call(
        functools.partial(exchange, n, groups),
        name="exchange",
        out_shape=(
            bf16((2, experts - TAIL, n * rows, width)),
            bf16((2 * TAIL, 2, rows, width)),
            *[bf16((2 * TAIL, rows, width)) for _ in away],
            jax.ShapeDtypeStruct((experts, width), jnp.float32),
            jax.ShapeDtypeStruct((experts, width), jnp.float32),
            bf16((groups * share, n * tokens)),
        ),
        in_specs=[anywhere, anywhere, inside, inside],
        out_specs=(anywhere,) * (2 + len(away)) + (inside, inside, anywhere),
        scratch_shapes=[
            pltpu.VMEM((depth, rows, columns), jnp.float32),
            pltpu.VMEM((SLOTS, n, rows, width), jnp.bfloat16),
            pltpu.VMEM((share, tokens), jnp.bfloat16),
            pltpu.VMEM((chips - 1, share, tokens), jnp.bfloat16),
            maxima,
            maxima,
            maxima,
            pltpu.VMEM((items, chips - 1, half, LANES), jnp.float32),
            maxima,
            pltpu.VMEM((n - 1, 2, half, LANES), jnp.float32),
            dma((depth,)),
            dma,
            dma((items,)),
            dma,
            dma((items,)),
            dma,
            dma((items,)),
            dma,
            dma,
            dma((SLOTS,)),
            dma((n - 1,)),
            dma((SLOTS,)),
            dma,
            dma,
            dma,
            dma((column,)),
            dma((column,)),
            dma,
        ],
        compiler_params=pltpu.CompilerParams(collective_id=0, has_side_effects=True),
    )(gate, up, router.T, gain.reshape(1, tokens))
    arrived = [
        lax.ppermute(ref, "shard", [(s, shift(s, d, f, chips)) for s in range(n)])
        for (d, f), ref in zip(away, far)
    ]
    finals = (bf16((experts, n * rows, width)),) * 2
    final = pl.pallas_call(
        spread,
        name="spread",
        grid=(experts - TAIL,),
        out_shape=finals,
        in_specs=[pl.BlockSpec((2, 1, n * rows, width), lambda e: (0, e, 0, 0))],
        out_specs=(pl.BlockSpec((1, n * rows, width), lambda e: (e, 0, 0)),) * 2,
        cost_estimate=pl.CostEstimate(flops=0, bytes_accessed=4 * narrow.size, transcendentals=0),
    )(narrow)

    def put(name, pieces, blocks, final, small=()):
        count = len(blocks) + len(small)
        return pl.pallas_call(
            functools.partial(finish, n, pieces, len(small)),
            name=name,
            out_shape=finals + tuple(jax.ShapeDtypeStruct(s.shape, s.dtype) for s in small),
            in_specs=[inside] * count + [anywhere] * 2,
            out_specs=(anywhere,) * 2 + (inside,) * len(small),
            scratch_shapes=[dma((len(blocks),))],
            input_output_aliases={count: 0, count + 1: 1},
            compiler_params=pltpu.CompilerParams(vmem_limit_bytes=16 * 2**20),
        )(*blocks, *small, *final)

    blocks = [jnp.expand_dims(ref, 1) for ref in arrived]
    *final, scale_gate, scale_up, routers = put(
        "finish_near", [None] + away[:-1], [near] + blocks[:-1], final,
        (scale_gate, scale_up, routers),
    )
    final_gate, final_up = put("finish_far", away[-1:], blocks[-1:], final)
    return final_gate, final_up, scale_gate, scale_up, routers.T


def by_collectives(gate, up, router, gain):
    scale_gate, scale_up = lax.pmax(
        (jnp.max(jnp.abs(gate), axis=1), jnp.max(jnp.abs(up), axis=1)), "shard"
    )

    def serve(master, scale):
        narrow = (master / jnp.expand_dims(scale, 1)).astype(jnp.bfloat16)
        final = lax.all_to_all(narrow, "shard", split_axis=2, concat_axis=1, tiled=True)
        width = final.shape[2]
        return final, lax.dynamic_slice_in_dim(
            scale, lax.axis_index("shard") * width, width, axis=1
        )

    final_gate, scale_gate = serve(gate, scale_gate)
    final_up, scale_up = serve(up, scale_up)
    part = (router * gain[:, None]).astype(jnp.bfloat16)
    rows = lax.all_gather(part, "shard", axis=0, tiled=True)
    return final_gate, final_up, scale_gate, scale_up, lax.all_gather(rows, "expert", axis=1, tiled=True)


def solution(mesh):
    n, groups = mesh.shape["shard"], mesh.shape["expert"]

    def shards(gate, up, router, gain):
        aligned = gate.shape[2] % (n * LANES) == 0 and gate.shape[1] % 16 == 0
        aligned = aligned and gate.shape[0] > TAIL + SLOTS + RAMP and 2 * TAIL <= SLOTS
        aligned = aligned and router.shape[0] % LANES == 0 and router.shape[1] % 16 == 0
        if n >= 4 and n % 2 == 0 and aligned:
            return by_kernel(n, groups, gate, up, router, gain)
        return by_collectives(gate, up, router, gain)

    return jax.shard_map(
        shards,
        mesh=mesh,
        in_specs=(
            P(("shift", "expert"), "shard", None),
            P(("shift", "expert"), "shard", None),
            P(("shift", "shard"), "expert"),
            P(("shift", "shard")),
        ),
        out_specs=(
            P(("shift", "expert"), None, "shard"),
            P(("shift", "expert"), None, "shard"),
            P(("shift", "expert"), "shard"),
            P(("shift", "expert"), "shard"),
            P("shift", None),
        ),
        check_vma=False,
    )
```

```python
import functools

import jax
import jax.numpy as jnp
from jax import lax
from jax.experimental import pallas as pl
from jax.experimental.pallas import tpu as pltpu
from jax.sharding import PartitionSpec as P

MESH = pl.DeviceIdType.MESH
LANES = 128
TAIL = 2
RAMP = 3
AHEAD = 3
SLOTS = 6


def shift(shard, d, f, chips):
    return 2 * ((shard // 2 + d) % chips) + (shard % 2 + f) % 2


def exchange(n, groups, gate, up, router, gain, *refs):
    chips = n // 2
    away = [(d, f) for d in range(1, chips) for f in (0, 1)]
    same, other = [p for p in away if p[1] == 0], [p for p in away if p[1] == 1]
    narrow, near, *far = refs[: 2 + len(away)]
    (
        scale_gate, scale_up, routers, held, out, part, passed, mine, beside, whole, cross, full,
        direct, load_sem, near_send, near_recv, cross_send, cross_recv, full_send, full_recv,
        direct_send, direct_recv, send_sem, recv_sem, keep_sem, tail_recv, pass_send, pass_recv,
        rt_send, rt_recv, rt_keep, go,
    ) = refs[2 + len(away) :]
    me, group = lax.axis_index("shard"), lax.axis_index("expert")
    core = lax.rem(me, 2)
    items, rows, width, depth = 2 * gate.shape[0], gate.shape[1], out.shape[3], held.shape[0]
    blocks, per, half = gate.shape[2] // LANES, width // LANES, gate.shape[2] // LANES // 2
    share, tokens = part.shape
    last = items - near.shape[0]
    column = [(f, g) for g in range(groups) for f in (0, 1) if (f, g) != (0, 0)]

    def peer(d, f):
        return 2 * lax.rem(me // 2 + d, chips) + lax.rem(core + f, 2)

    def device(d, f, g=0):
        return {"shard": peer(d, f), "expert": lax.rem(group + g, groups)}

    def remote(src, dst, send, recv, to):
        return pltpu.make_async_remote_copy(
            src, dst, send, recv, device_id=to, device_id_type=MESH
        )

    def await_bytes(ref, sem):
        pltpu.make_async_copy(ref, ref, sem).wait()

    def load(k):
        slot, expert = lax.rem(k, depth), k // 2

        @pl.when(lax.rem(k, 2) == 0)
        def _():
            pltpu.make_async_copy(gate.at[expert], held.at[slot], load_sem.at[slot]).start()

        @pl.when(lax.rem(k, 2) == 1)
        def _():
            pltpu.make_async_copy(up.at[expert], held.at[slot], load_sem.at[slot]).start()

    def local(k):
        slot = lax.rem(k, depth)
        await_bytes(held.at[slot], load_sem.at[slot])
        for b in range(blocks):
            values = held[slot, :, b * LANES : (b + 1) * LANES]
            mine[k, b // half, b % half : b % half + 1, :] = jnp.max(
                jnp.abs(values), axis=0, keepdims=True
            )

    def tell(k):
        remote(mine.at[k], beside.at[k], near_send, near_recv.at[k], device(0, 1)).start()

    def ask(k):
        await_bytes(beside.at[k], near_recv.at[k])
        whole[k] = jnp.maximum(mine[k], beside[k])
        for d in range(1, chips):
            remote(
                whole.at[k, core], cross.at[k, d - 1], cross_send, cross_recv.at[k], device(d, 0)
            ).start()

    def relay(k):
        await_bytes(cross.at[k], cross_recv.at[k])
        most = whole[k, core]
        for d in range(1, chips):
            most = jnp.maximum(most, cross[k, d - 1])
        full[k, core] = most
        remote(full.at[k, core], full.at[k, core], full_send, full_recv.at[k], device(0, 1)).start()

    def place(k):
        return narrow.at[lax.rem(k, 2), k // 2, pl.ds(pl.multiple_of(me * rows, rows), rows)]

    def send(k, pieces):
        slot = lax.rem(k, SLOTS)
        for d, f in pieces:
            remote(
                out.at[slot, peer(d, f)], place(k), send_sem.at[slot],
                recv_sem.at[2 * d + f - 1], device(d, f),
            ).start()

    def keep(k):
        slot = lax.rem(k, SLOTS)
        send(k, [(0, 1)])
        pltpu.make_async_copy(out.at[slot, me], place(k), keep_sem.at[slot]).start()

    def sent(k):
        slot = lax.rem(k, SLOTS)
        await_bytes(out.at[slot, pl.ds(0, n - 1)], send_sem.at[slot])
        await_bytes(out.at[slot, 0], keep_sem.at[slot])

    def leave(k):
        slot, i = lax.rem(k, SLOTS), k - last
        remote(
            out.at[slot, peer(0, 1)], near.at[i, core], send_sem.at[slot], tail_recv, device(0, 1)
        ).start()
        pltpu.make_async_copy(out.at[slot, me], near.at[i, core], keep_sem.at[slot]).start()
        for (d, f), ref in zip(away, far):
            pltpu.make_async_copy(out.at[slot, peer(d, f)], ref.at[i], keep_sem.at[slot]).start()

    def left(k):
        slot = lax.rem(k, SLOTS)
        await_bytes(out.at[slot, 0], send_sem.at[slot])
        await_bytes(out.at[slot, pl.ds(0, n - 1)], keep_sem.at[slot])

    def home(shard):
        return routers.at[
            pl.ds(pl.multiple_of(group * share, share), share),
            pl.ds(pl.multiple_of(shard * tokens, tokens), tokens),
        ]

    def spread_router(block, shard):
        for i, (f, g) in enumerate(column):
            remote(block, home(shard), rt_send.at[i], rt_recv.at[i], device(0, f, g)).start()
        pltpu.make_async_copy(block, home(shard), rt_keep).start()

    for k in range(AHEAD):
        load(jnp.int32(k))
    barrier = pltpu.get_barrier_semaphore()
    for to in [device(d, f) for d, f in away] + [device(0, f, g) for f, g in column]:
        pl.semaphore_signal(barrier, inc=1, device_id=to, device_id_type=MESH)
    part[...] = (router[...] * gain[...]).astype(jnp.bfloat16)
    local(0)
    load(jnp.int32(AHEAD))
    pl.semaphore_wait(barrier, len(away) + len(column))
    for j, (d, f) in enumerate(away + [(0, 1)]):
        remote(mine.at[0], direct.at[j], direct_send, direct_recv, device(d, f)).start()
    for d in range(1, chips):
        remote(part, passed.at[d - 1], pass_send, pass_recv, device(d, 0)).start()
    spread_router(part, me)
    local(1)
    load(jnp.int32(AHEAD + 1))
    tell(1)
    ask(1)
    await_bytes(direct, direct_recv)
    most = mine[0]
    for j in range(n - 1):
        most = jnp.maximum(most, direct[j])
    full[0] = most

    def step(q, _):
        @pl.when(q > 0)
        def _():
            await_bytes(full.at[q, 0], full_recv.at[q])

        @pl.when((q > SLOTS) | ((q == SLOTS) & (core == 1)))
        def _():
            sent(q - SLOTS)

        slot, source = lax.rem(q, SLOTS), lax.rem(q, depth)
        for b in range(blocks):
            at = (b % per) * LANES
            values = held[source, :, b * LANES : (b + 1) * LANES]
            scale = full[q, b // half, b % half : b % half + 1, :]
            out[slot, b // per, :, at : at + LANES] = (values / scale).astype(jnp.bfloat16)

        @pl.when((q < last) & (core == 0))
        def _():
            send(q, same + other)

        @pl.when(q < last)
        def _():
            keep(q)

        @pl.when(q >= last)
        def _():
            leave(q)

        first = q + jnp.minimum(q, RAMP) + 2
        leads = [(first, first < items), (first + 1, q < RAMP)]
        for k, due in leads:
            @pl.when(due)
            def _():
                local(k)
                tell(k)

                @pl.when(k + AHEAD < items)
                def _():
                    load(k + AHEAD)

        for k, due in leads:
            @pl.when(due)
            def _():
                ask(k)

        @pl.when(q + 1 < items)
        def _():
            relay(q + 1)

        @pl.when((q == 1) & (core == 0))
        def _():
            sent(0)
            pl.semaphore_signal(go, inc=1, device_id=device(0, 1), device_id_type=MESH)

        @pl.when((q == 1) & (core == 1))
        def _():
            pl.semaphore_wait(go, 1)
            send(0, other)

        @pl.when((q > 0) & (q < last) & (core == 1))
        def _():
            send(q, other)

        @pl.when((q > 0) & (q <= last) & (core == 1))
        def _():
            send(q - 1, same)

        @pl.when(q == RAMP)
        def _():
            await_bytes(passed, pass_recv)
            for d in range(1, chips):
                spread_router(passed.at[d - 1], peer(chips - d, 0))

        return 0

    lax.fori_loop(0, items, step, 0)

    for e in range(items // 2):
        for which, ref in enumerate((scale_gate, scale_up)):
            for i in range(per):
                b = me * per + i
                ref[e : e + 1, i * LANES : (i + 1) * LANES] = full[
                    2 * e + which, b // half, pl.ds(lax.rem(b, half), 1), :
                ]

    def drain(k, _):
        sent(k)
        return 0

    lax.fori_loop(items - SLOTS, last, drain, 0)

    def drain_tail(k, _):
        left(k)
        return 0

    lax.fori_loop(last, items, drain_tail, 0)
    await_bytes(beside.at[pl.ds(1, items - 1)], near_send)
    await_bytes(cross.at[pl.ds(1, items - 1)], cross_send)
    await_bytes(full.at[pl.ds(1, items - 1), 0], full_send)
    await_bytes(direct, direct_send)
    await_bytes(passed, pass_send)
    strip = routers.at[pl.ds(0, share), pl.ds(0, chips * tokens)]
    for i in range(len(column)):
        await_bytes(strip, rt_send.at[i])
        await_bytes(strip, rt_recv.at[i])
    await_bytes(strip, rt_keep)
    await_bytes(near.at[:, 0], tail_recv)
    for j in range(n - 1):
        await_bytes(narrow.at[:, :, pl.ds(0, rows)], recv_sem.at[j])


def spread(narrow, gate, up):
    gate[...] = narrow[0]
    up[...] = narrow[1]


def finish(n, pieces, extras, *refs):
    count = len(pieces)
    arrived, small, results, sems = (
        refs[:count], refs[count : count + extras], refs[count + extras + 2 : -1], refs[-1]
    )
    gate, up, *copies = results
    me, chips = lax.axis_index("shard"), n // 2
    experts, tail, rows = gate.shape[0], arrived[0].shape[0], gate.shape[1] // n
    for at, (piece, ref) in enumerate(zip(pieces, arrived)):
        for i in range(tail):
            final = (gate, up)[i % 2].at[experts - tail // 2 + i // 2]
            for c in range(ref.shape[1]):
                if piece is None:
                    source = 2 * (me // 2) + c
                else:
                    d, f = piece
                    source = 2 * lax.rem(me // 2 + chips - d, chips) + lax.rem(me % 2 + f, 2)
                to = final.at[pl.ds(pl.multiple_of(source * rows, rows), rows)]
                pltpu.make_async_copy(ref.at[i, c], to, sems.at[at]).start()
    for ref, copy in zip(small, copies):
        copy[...] = ref[...]
    for at, ref in enumerate(arrived):
        pltpu.make_async_copy(ref, ref, sems.at[at]).wait()


def by_kernel(n, groups, gate, up, router, gain):
    experts, rows, columns = gate.shape
    width, items, depth, chips = columns // n, 2 * experts, RAMP + AHEAD + 2, n // 2
    tokens, share = router.shape
    half = columns // LANES // 2
    away = [(d, f) for d in range(1, chips) for f in (0, 1)]
    column = 2 * groups - 1
    anywhere = pl.BlockSpec(memory_space=pl.ANY)
    inside = pl.BlockSpec(memory_space=pltpu.VMEM)
    dma = pltpu.SemaphoreType.DMA
    bf16 = functools.partial(jax.ShapeDtypeStruct, dtype=jnp.bfloat16)
    maxima = pltpu.VMEM((items, 2, half, LANES), jnp.float32)
    narrow, near, *far, scale_gate, scale_up, routers = pl.pallas_call(
        functools.partial(exchange, n, groups),
        name="exchange",
        out_shape=(
            bf16((2, experts - TAIL, n * rows, width)),
            bf16((2 * TAIL, 2, rows, width)),
            *[bf16((2 * TAIL, rows, width)) for _ in away],
            jax.ShapeDtypeStruct((experts, width), jnp.float32),
            jax.ShapeDtypeStruct((experts, width), jnp.float32),
            bf16((groups * share, n * tokens)),
        ),
        in_specs=[anywhere, anywhere, inside, inside],
        out_specs=(anywhere,) * (2 + len(away)) + (inside, inside, anywhere),
        scratch_shapes=[
            pltpu.VMEM((depth, rows, columns), jnp.float32),
            pltpu.VMEM((SLOTS, n, rows, width), jnp.bfloat16),
            pltpu.VMEM((share, tokens), jnp.bfloat16),
            pltpu.VMEM((chips - 1, share, tokens), jnp.bfloat16),
            maxima,
            maxima,
            maxima,
            pltpu.VMEM((items, chips - 1, half, LANES), jnp.float32),
            maxima,
            pltpu.VMEM((n - 1, 2, half, LANES), jnp.float32),
            dma((depth,)),
            dma,
            dma((items,)),
            dma,
            dma((items,)),
            dma,
            dma((items,)),
            dma,
            dma,
            dma((SLOTS,)),
            dma((n - 1,)),
            dma((SLOTS,)),
            dma,
            dma,
            dma,
            dma((column,)),
            dma((column,)),
            dma,
            pltpu.SemaphoreType.REGULAR,
        ],
        compiler_params=pltpu.CompilerParams(collective_id=0, has_side_effects=True),
    )(gate, up, router.T, gain.reshape(1, tokens))
    arrived = [
        lax.ppermute(ref, "shard", [(s, shift(s, d, f, chips)) for s in range(n)])
        for (d, f), ref in zip(away, far)
    ]
    finals = (bf16((experts, n * rows, width)),) * 2
    final = pl.pallas_call(
        spread,
        name="spread",
        grid=(experts - TAIL,),
        out_shape=finals,
        in_specs=[pl.BlockSpec((2, 1, n * rows, width), lambda e: (0, e, 0, 0))],
        out_specs=(pl.BlockSpec((1, n * rows, width), lambda e: (e, 0, 0)),) * 2,
        cost_estimate=pl.CostEstimate(flops=0, bytes_accessed=4 * narrow.size, transcendentals=0),
    )(narrow)

    def put(name, pieces, blocks, final, small=()):
        count = len(blocks) + len(small)
        return pl.pallas_call(
            functools.partial(finish, n, pieces, len(small)),
            name=name,
            out_shape=finals + tuple(jax.ShapeDtypeStruct(s.shape, s.dtype) for s in small),
            in_specs=[inside] * count + [anywhere] * 2,
            out_specs=(anywhere,) * 2 + (inside,) * len(small),
            scratch_shapes=[dma((len(blocks),))],
            input_output_aliases={count: 0, count + 1: 1},
            compiler_params=pltpu.CompilerParams(vmem_limit_bytes=16 * 2**20),
        )(*blocks, *small, *final)

    blocks = [jnp.expand_dims(ref, 1) for ref in arrived]
    *final, scale_gate, scale_up, routers = put(
        "finish_near", [None] + away[:-1], [near] + blocks[:-1], final,
        (scale_gate, scale_up, routers),
    )
    final_gate, final_up = put("finish_far", away[-1:], blocks[-1:], final)
    return final_gate, final_up, scale_gate, scale_up, routers.T


def by_collectives(gate, up, router, gain):
    scale_gate, scale_up = lax.pmax(
        (jnp.max(jnp.abs(gate), axis=1), jnp.max(jnp.abs(up), axis=1)), "shard"
    )

    def serve(master, scale):
        narrow = (master / jnp.expand_dims(scale, 1)).astype(jnp.bfloat16)
        final = lax.all_to_all(narrow, "shard", split_axis=2, concat_axis=1, tiled=True)
        width = final.shape[2]
        return final, lax.dynamic_slice_in_dim(
            scale, lax.axis_index("shard") * width, width, axis=1
        )

    final_gate, scale_gate = serve(gate, scale_gate)
    final_up, scale_up = serve(up, scale_up)
    part = (router * gain[:, None]).astype(jnp.bfloat16)
    rows = lax.all_gather(part, "shard", axis=0, tiled=True)
    return final_gate, final_up, scale_gate, scale_up, lax.all_gather(rows, "expert", axis=1, tiled=True)


def solution(mesh):
    n, groups = mesh.shape["shard"], mesh.shape["expert"]

    def shards(gate, up, router, gain):
        aligned = gate.shape[2] % (n * LANES) == 0 and gate.shape[1] % 16 == 0
        aligned = aligned and gate.shape[0] > TAIL + SLOTS + RAMP and 2 * TAIL <= SLOTS
        aligned = aligned and router.shape[0] % LANES == 0 and router.shape[1] % 16 == 0
        if n >= 4 and n % 2 == 0 and aligned:
            return by_kernel(n, groups, gate, up, router, gain)
        return by_collectives(gate, up, router, gain)

    return jax.shard_map(
        shards,
        mesh=mesh,
        in_specs=(
            P(("shift", "expert"), "shard", None),
            P(("shift", "expert"), "shard", None),
            P(("shift", "shard"), "expert"),
            P(("shift", "shard")),
        ),
        out_specs=(
            P(("shift", "expert"), None, "shard"),
            P(("shift", "expert"), None, "shard"),
            P(("shift", "expert"), "shard"),
            P(("shift", "expert"), "shard"),
            P("shift", None),
        ),
        check_vma=False,
    )
```

```python
import functools

import jax
import jax.numpy as jnp
from jax import lax
from jax.experimental import pallas as pl
from jax.experimental.pallas import tpu as pltpu
from jax.sharding import PartitionSpec as P

MESH = pl.DeviceIdType.MESH
LANES = 128
TAIL = 2
RAMP = 3
AHEAD = 3
SLOTS = 6
CHUNKS = 4


def shift(shard, d, f, chips):
    return 2 * ((shard // 2 + d) % chips) + (shard % 2 + f) % 2


def exchange(n, gate, up, router, gain, *refs):
    chips = n // 2
    away = [(d, f) for d in range(1, chips) for f in (0, 1)]
    same, other = [p for p in away if p[1] == 0], [p for p in away if p[1] == 1]
    narrow, near, *far = refs[: 2 + len(away)]
    (
        scale_gate, scale_up, pair, held, out, weight, by, part, scales, mine, beside, whole, cross,
        full, direct, first_sem, load_sem, near_send, near_recv, cross_send, cross_recv, full_send,
        full_recv, direct_send, direct_recv, send_sem, recv_sem, keep_sem, tail_recv, small_sem,
        pass_send, pass_recv, scale_sem, go,
    ) = refs[2 + len(away) :]
    me = lax.axis_index("shard")
    core = lax.rem(me, 2)
    items, rows, width, depth = 2 * gate.shape[0], gate.shape[1], out.shape[3], held.shape[0]
    blocks, per, half = gate.shape[2] // LANES, width // LANES, gate.shape[2] // LANES // 2
    last, chunk = items - near.shape[0], rows // CHUNKS

    def peer(d, f):
        return 2 * lax.rem(me // 2 + d, chips) + lax.rem(core + f, 2)

    def device(d, f):
        return {"shard": peer(d, f)}

    def remote(src, dst, send, recv, to):
        return pltpu.make_async_remote_copy(
            src, dst, send, recv, device_id=to, device_id_type=MESH
        )

    def await_bytes(ref, sem):
        pltpu.make_async_copy(ref, ref, sem).wait()

    def load(k):
        slot, expert = lax.rem(k, depth), k // 2

        @pl.when(lax.rem(k, 2) == 0)
        def _():
            pltpu.make_async_copy(gate.at[expert], held.at[slot], load_sem.at[slot]).start()

        @pl.when(lax.rem(k, 2) == 1)
        def _():
            pltpu.make_async_copy(up.at[expert], held.at[slot], load_sem.at[slot]).start()

    def first(c):
        at = pl.ds(c * chunk, chunk)
        return pltpu.make_async_copy(gate.at[0, at], held.at[0, at], first_sem.at[c])

    def local(k):
        slot = lax.rem(k, depth)
        await_bytes(held.at[slot], load_sem.at[slot])
        for b in range(blocks):
            values = held[slot, :, b * LANES : (b + 1) * LANES]
            mine[k, b // half, b % half : b % half + 1, :] = jnp.max(
                jnp.abs(values), axis=0, keepdims=True
            )

    def scaled(k, shard):
        slot, source = lax.rem(k, SLOTS), lax.rem(k, depth)
        for i in range(per):
            b = shard * per + i
            values = held[source, :, pl.ds(pl.multiple_of(b * LANES, LANES), LANES)]
            scale = full[k, b // half, pl.ds(lax.rem(b, half), 1), :]
            out[slot, shard, :, i * LANES : (i + 1) * LANES] = (values / scale).astype(
                jnp.bfloat16
            )

    def tell(k):
        remote(mine.at[k], beside.at[k], near_send, near_recv.at[k], device(0, 1)).start()

    def ask(k):
        await_bytes(beside.at[k], near_recv.at[k])
        whole[k] = jnp.maximum(mine[k], beside[k])
        for d in range(1, chips):
            remote(
                whole.at[k, core], cross.at[k, d - 1], cross_send, cross_recv.at[k], device(d, 0)
            ).start()

    def relay(k):
        await_bytes(cross.at[k], cross_recv.at[k])
        most = whole[k, core]
        for d in range(1, chips):
            most = jnp.maximum(most, cross[k, d - 1])
        full[k, core] = most
        remote(full.at[k, core], full.at[k, core], full_send, full_recv.at[k], device(0, 1)).start()

    def place(k):
        return narrow.at[lax.rem(k, 2), k // 2, pl.ds(pl.multiple_of(me * rows, rows), rows)]

    def send(k, pieces):
        slot = lax.rem(k, SLOTS)
        for d, f in pieces:
            remote(
                out.at[slot, peer(d, f)], place(k), send_sem.at[slot],
                recv_sem.at[2 * d + f - 1], device(d, f),
            ).start()

    def keep(k):
        slot = lax.rem(k, SLOTS)
        send(k, [(0, 1)])
        pltpu.make_async_copy(out.at[slot, me], place(k), keep_sem.at[slot]).start()

    def sent(k):
        slot = lax.rem(k, SLOTS)
        await_bytes(out.at[slot, pl.ds(0, n - 1)], send_sem.at[slot])
        await_bytes(out.at[slot, 0], keep_sem.at[slot])

    def leave(k):
        slot, i = lax.rem(k, SLOTS), k - last
        remote(
            out.at[slot, peer(0, 1)], near.at[i, core], send_sem.at[slot], tail_recv, device(0, 1)
        ).start()
        pltpu.make_async_copy(out.at[slot, me], near.at[i, core], keep_sem.at[slot]).start()
        for (d, f), ref in zip(away, far):
            pltpu.make_async_copy(out.at[slot, peer(d, f)], ref.at[i], keep_sem.at[slot]).start()

    def left(k):
        slot = lax.rem(k, SLOTS)
        await_bytes(out.at[slot, 0], send_sem.at[slot])
        await_bytes(out.at[slot, pl.ds(0, n - 1)], keep_sem.at[slot])

    for c in range(CHUNKS):
        first(c).start()
    barrier = pltpu.get_barrier_semaphore()
    for d, f in away + [(0, 1)]:
        pl.semaphore_signal(barrier, inc=1, device_id=device(d, f), device_id_type=MESH)
    small = [
        pltpu.make_async_copy(router, weight, small_sem.at[0]),
        pltpu.make_async_copy(gain, by, small_sem.at[1]),
    ]
    for c in range(CHUNKS):
        first(c).wait()
        if c == 0:
            load(jnp.int32(1))
        for b in range(blocks):
            values = held[0, c * chunk : (c + 1) * chunk, b * LANES : (b + 1) * LANES]
            most = jnp.max(jnp.abs(values), axis=0, keepdims=True)
            at = b // half, slice(b % half, b % half + 1)
            mine[(0, *at)] = most if c == 0 else jnp.maximum(mine[(0, *at)], most)
    for k in range(2, AHEAD + 1):
        load(jnp.int32(k))
    for copy in small:
        copy.start()
    pl.semaphore_wait(barrier, n - 1)
    for j, (d, f) in enumerate(away + [(0, 1)]):
        remote(mine.at[0], direct.at[j], direct_send, direct_recv, device(d, f)).start()
    local(1)
    load(jnp.int32(AHEAD + 1))
    tell(1)
    for copy in small:
        copy.wait()
    part[...] = (weight[...] * by[...]).astype(jnp.bfloat16)
    ask(1)
    await_bytes(direct, direct_recv)
    most = mine[0]
    for j in range(n - 1):
        most = jnp.maximum(most, direct[j])
    full[0] = most

    def step(q, _):
        @pl.when(q > 0)
        def _():
            await_bytes(full.at[q, 0], full_recv.at[q])

        @pl.when((q > SLOTS) | ((q == SLOTS) & (core == 1)))
        def _():
            sent(q - SLOTS)

        before = None
        for d, f in away + [(0, 1), (0, 0)]:
            scaled(q, peer(d, f))
            if before is not None:
                @pl.when((q < last) & (core == 0))
                def _():
                    send(q, [before])

            before = (d, f) if d > 0 else None

        @pl.when(q < last)
        def _():
            keep(q)

        @pl.when(q >= last)
        def _():
            leave(q)

        first = q + jnp.minimum(q, RAMP) + 2
        leads = [(first, first < items), (first + 1, q < RAMP)]
        for k, due in leads:
            @pl.when(due)
            def _():
                local(k)
                tell(k)

                @pl.when(k + AHEAD < items)
                def _():
                    load(k + AHEAD)

        for k, due in leads:
            @pl.when(due)
            def _():
                ask(k)

        @pl.when(q + 1 < items)
        def _():
            relay(q + 1)

        @pl.when((q == 1) & (core == 0))
        def _():
            sent(0)
            pl.semaphore_signal(go, inc=1, device_id=device(0, 1), device_id_type=MESH)

        @pl.when((q == 1) & (core == 1))
        def _():
            pl.semaphore_wait(go, 1)
            send(0, other)

        @pl.when((q > 0) & (q < last) & (core == 1))
        def _():
            send(q, other)

        @pl.when((q > 0) & (q <= last) & (core == 1))
        def _():
            send(q - 1, same)

        @pl.when(q == RAMP)
        def _():
            pltpu.make_async_copy(part, pair.at[0], small_sem.at[0]).start()
            for d in range(1, chips):
                remote(part, pair.at[d], pass_send, pass_recv, device(d, 0)).start()

        return 0

    lax.fori_loop(0, items, step, 0)

    for e in range(items // 2):
        for which in (0, 1):
            for i in range(per):
                b = me * per + i
                scales[which, e : e + 1, i * LANES : (i + 1) * LANES] = full[
                    2 * e + which, b // half, pl.ds(lax.rem(b, half), 1), :
                ]

    for which, ref in enumerate((scale_gate, scale_up)):
        pltpu.make_async_copy(scales.at[which], ref, scale_sem.at[which]).start()

    def drain(k, _):
        sent(k)
        return 0

    lax.fori_loop(items - SLOTS, last, drain, 0)

    def drain_tail(k, _):
        left(k)
        return 0

    lax.fori_loop(last, items, drain_tail, 0)
    await_bytes(beside.at[pl.ds(1, items - 1)], near_send)
    await_bytes(cross.at[pl.ds(1, items - 1)], cross_send)
    await_bytes(full.at[pl.ds(1, items - 1), 0], full_send)
    await_bytes(direct, direct_send)
    rest = pair.at[pl.ds(1, chips - 1)]
    await_bytes(rest, pass_send)
    await_bytes(rest, pass_recv)
    await_bytes(part, small_sem.at[0])
    for which in (0, 1):
        await_bytes(scales.at[which], scale_sem.at[which])
    await_bytes(near.at[:, 0], tail_recv)
    for j in range(n - 1):
        await_bytes(narrow.at[:, :, pl.ds(0, rows)], recv_sem.at[j])


def gather(n, groups, token, pair, routers, send_sem, recv_sem, keep_sem):
    del token
    me, group, chips = lax.axis_index("shard"), lax.axis_index("expert"), n // 2
    core, (_, share, tokens) = lax.rem(me, 2), pair.shape
    column = [(f, g) for g in range(groups) for f in (0, 1) if (f, g) != (0, 0)]

    def device(f, g):
        near = me - core + lax.rem(core + f, 2)
        return {"shard": near, "expert": lax.rem(group + g, groups)}

    barrier = pltpu.get_barrier_semaphore()
    for f, g in column:
        pl.semaphore_signal(barrier, inc=1, device_id=device(f, g), device_id_type=MESH)
    pl.semaphore_wait(barrier, len(column))
    for d in range(chips):
        shard = 2 * lax.rem(me // 2 + chips - d, chips) + core
        home = routers.at[
            pl.ds(pl.multiple_of(group * share, share), share),
            pl.ds(pl.multiple_of(shard * tokens, tokens), tokens),
        ]
        for i, (f, g) in enumerate(column):
            pltpu.make_async_remote_copy(
                pair.at[d], home, send_sem.at[i], recv_sem.at[i],
                device_id=device(f, g), device_id_type=MESH,
            ).start()
        pltpu.make_async_copy(pair.at[d], home, keep_sem).start()
    for i in range(len(column)):
        pltpu.make_async_copy(pair, pair, send_sem.at[i]).wait()
        pltpu.make_async_copy(pair, pair, recv_sem.at[i]).wait()
    pltpu.make_async_copy(pair, pair, keep_sem).wait()


def spread(narrow, gate, up, token):
    gate[...] = narrow[0]
    up[...] = narrow[1]
    token[...] = jnp.zeros_like(token)


def finish(n, pieces, extras, *refs):
    count = len(pieces)
    arrived, small, results, sems = (
        refs[:count], refs[count : count + extras], refs[count + extras + 2 : -1], refs[-1]
    )
    gate, up, *copies = results
    me, chips = lax.axis_index("shard"), n // 2
    experts, tail, rows = gate.shape[0], arrived[0].shape[0], gate.shape[1] // n
    for at, (piece, ref) in enumerate(zip(pieces, arrived)):
        for i in range(tail):
            final = (gate, up)[i % 2].at[experts - tail // 2 + i // 2]
            for c in range(ref.shape[1]):
                if piece is None:
                    source = 2 * (me // 2) + c
                else:
                    d, f = piece
                    source = 2 * lax.rem(me // 2 + chips - d, chips) + lax.rem(me % 2 + f, 2)
                to = final.at[pl.ds(pl.multiple_of(source * rows, rows), rows)]
                pltpu.make_async_copy(ref.at[i, c], to, sems.at[at]).start()
    for ref, copy in zip(small, copies):
        copy[...] = ref[...]
    for at, ref in enumerate(arrived):
        pltpu.make_async_copy(ref, ref, sems.at[at]).wait()


def by_kernel(n, groups, gate, up, router, gain):
    experts, rows, columns = gate.shape
    width, items, depth, chips = columns // n, 2 * experts, RAMP + AHEAD + 2, n // 2
    tokens, share = router.shape
    half = columns // LANES // 2
    away = [(d, f) for d in range(1, chips) for f in (0, 1)]
    column = 2 * groups - 1
    f32 = functools.partial(jax.ShapeDtypeStruct, dtype=jnp.float32)
    anywhere = pl.BlockSpec(memory_space=pl.ANY)
    inside = pl.BlockSpec(memory_space=pltpu.VMEM)
    dma = pltpu.SemaphoreType.DMA
    bf16 = functools.partial(jax.ShapeDtypeStruct, dtype=jnp.bfloat16)
    maxima = pltpu.VMEM((items, 2, half, LANES), jnp.float32)
    narrow, near, *far, scale_gate, scale_up, pair = pl.pallas_call(
        functools.partial(exchange, n),
        name="exchange",
        out_shape=(
            bf16((2, experts - TAIL, n * rows, width)),
            bf16((2 * TAIL, 2, rows, width)),
            *[bf16((2 * TAIL, rows, width)) for _ in away],
            f32((experts, width)),
            f32((experts, width)),
            bf16((chips, share, tokens)),
        ),
        in_specs=[anywhere] * 4,
        out_specs=(anywhere,) * (5 + len(away)),
        scratch_shapes=[
            pltpu.VMEM((depth, rows, columns), jnp.float32),
            pltpu.VMEM((SLOTS, n, rows, width), jnp.bfloat16),
            pltpu.VMEM((share, tokens), jnp.float32),
            pltpu.VMEM((1, tokens), jnp.float32),
            pltpu.VMEM((share, tokens), jnp.bfloat16),
            pltpu.VMEM((2, experts, width), jnp.float32),
            maxima,
            maxima,
            maxima,
            pltpu.VMEM((items, chips - 1, half, LANES), jnp.float32),
            maxima,
            pltpu.VMEM((n - 1, 2, half, LANES), jnp.float32),
            dma((CHUNKS,)),
            dma((depth,)),
            dma,
            dma((items,)),
            dma,
            dma((items,)),
            dma,
            dma((items,)),
            dma,
            dma,
            dma((SLOTS,)),
            dma((n - 1,)),
            dma((SLOTS,)),
            dma,
            dma((2,)),
            dma,
            dma,
            dma((2,)),
            pltpu.SemaphoreType.REGULAR,
        ],
        compiler_params=pltpu.CompilerParams(collective_id=0, has_side_effects=True),
    )(gate, up, router.T, gain.reshape(1, tokens))
    arrived = [
        lax.ppermute(ref, "shard", [(s, shift(s, d, f, chips)) for s in range(n)])
        for (d, f), ref in zip(away, far)
    ]
    finals = (bf16((experts, n * rows, width)),) * 2
    *final, token = pl.pallas_call(
        spread,
        name="spread",
        grid=(experts - TAIL,),
        out_shape=finals + (f32((8, LANES)),),
        in_specs=[pl.BlockSpec((2, 1, n * rows, width), lambda e: (0, e, 0, 0))],
        out_specs=(pl.BlockSpec((1, n * rows, width), lambda e: (e, 0, 0)),) * 2
        + (pl.BlockSpec((8, LANES), lambda e: (0, 0)),),
        cost_estimate=pl.CostEstimate(flops=0, bytes_accessed=4 * narrow.size, transcendentals=0),
    )(narrow)

    routers = pl.pallas_call(
        functools.partial(gather, n, groups),
        name="gather",
        out_shape=bf16((groups * share, n * tokens)),
        in_specs=[anywhere, inside],
        out_specs=anywhere,
        scratch_shapes=[dma((column,)), dma((column,)), dma],
        compiler_params=pltpu.CompilerParams(
            collective_id=1, has_side_effects=True, vmem_limit_bytes=16 * 2**20
        ),
    )(token, pair)

    def put(name, pieces, blocks, final, small=()):
        count = len(blocks) + len(small)
        return pl.pallas_call(
            functools.partial(finish, n, pieces, len(small)),
            name=name,
            out_shape=finals + tuple(jax.ShapeDtypeStruct(s.shape, s.dtype) for s in small),
            in_specs=[inside] * count + [anywhere] * 2,
            out_specs=(anywhere,) * 2 + (inside,) * len(small),
            scratch_shapes=[dma((len(blocks),))],
            input_output_aliases={count: 0, count + 1: 1},
            compiler_params=pltpu.CompilerParams(vmem_limit_bytes=16 * 2**20),
        )(*blocks, *small, *final)

    blocks = [jnp.expand_dims(ref, 1) for ref in arrived]
    *final, scale_gate, scale_up, routers = put(
        "finish_near", [None] + away[:-1], [near] + blocks[:-1], final,
        (scale_gate, scale_up, routers),
    )
    final_gate, final_up = put("finish_far", away[-1:], blocks[-1:], final)
    return final_gate, final_up, scale_gate, scale_up, routers.T


def by_collectives(gate, up, router, gain):
    scale_gate, scale_up = lax.pmax(
        (jnp.max(jnp.abs(gate), axis=1), jnp.max(jnp.abs(up), axis=1)), "shard"
    )

    def serve(master, scale):
        narrow = (master / jnp.expand_dims(scale, 1)).astype(jnp.bfloat16)
        final = lax.all_to_all(narrow, "shard", split_axis=2, concat_axis=1, tiled=True)
        width = final.shape[2]
        return final, lax.dynamic_slice_in_dim(
            scale, lax.axis_index("shard") * width, width, axis=1
        )

    final_gate, scale_gate = serve(gate, scale_gate)
    final_up, scale_up = serve(up, scale_up)
    part = (router * gain[:, None]).astype(jnp.bfloat16)
    rows = lax.all_gather(part, "shard", axis=0, tiled=True)
    return final_gate, final_up, scale_gate, scale_up, lax.all_gather(rows, "expert", axis=1, tiled=True)


def solution(mesh):
    n, groups = mesh.shape["shard"], mesh.shape["expert"]

    def shards(gate, up, router, gain):
        aligned = gate.shape[2] % (n * LANES) == 0 and gate.shape[1] % (16 * CHUNKS) == 0
        aligned = aligned and gate.shape[0] > TAIL + SLOTS + RAMP and 2 * TAIL <= SLOTS
        aligned = aligned and router.shape[0] % LANES == 0 and router.shape[1] % 16 == 0
        if n >= 4 and n % 2 == 0 and aligned:
            return by_kernel(n, groups, gate, up, router, gain)
        return by_collectives(gate, up, router, gain)

    return jax.shard_map(
        shards,
        mesh=mesh,
        in_specs=(
            P(("shift", "expert"), "shard", None),
            P(("shift", "expert"), "shard", None),
            P(("shift", "shard"), "expert"),
            P(("shift", "shard")),
        ),
        out_specs=(
            P(("shift", "expert"), None, "shard"),
            P(("shift", "expert"), None, "shard"),
            P(("shift", "expert"), "shard"),
            P(("shift", "expert"), "shard"),
            P("shift", None),
        ),
        check_vma=False,
    )
```

```python
import functools

import jax
import jax.numpy as jnp
from jax import lax
from jax.experimental import pallas as pl
from jax.experimental.pallas import tpu as pltpu
from jax.sharding import PartitionSpec as P


MESH = pl.DeviceIdType.MESH
LANES = 128
TAIL = 2
EARLY = 3
RAMP = 3
AHEAD = 3
SLOTS = 6
CHUNKS = 4
EIGHTH = 8


def shift(shard, d, f, chips):
    return 2 * ((shard // 2 + d) % chips) + (shard % 2 + f) % 2


def tail_pieces(n):
    ahead = range(1, n // 2)
    return (
        [(d, 0, 0, EARLY) for d in ahead]
        + [(d, 1, 0, 2 * TAIL) for d in ahead]
        + [(d, 0, EARLY, 2 * TAIL - EARLY) for d in ahead]
    )


def exchange(n, gate, up, router, gain, *refs):
    chips = n // 2
    away = [(d, f) for d in range(1, chips) for f in (0, 1)]
    same, other = [p for p in away if p[1] == 0], [p for p in away if p[1] == 1]
    pieces = tail_pieces(n)
    narrow, near, *far = refs[: 2 + len(pieces)]
    (
        scale_gate, scale_up, pair, held, out, weight, by, part, scales, mine, beside, whole, cross,
        full, direct, raw, late, first_sem, load_sem, near_send, near_recv, cross_send, cross_recv, full_send,
        full_recv, direct_send, direct_recv, send_sem, recv_sem, keep_sem, tail_recv, small_sem,
        pass_send, pass_recv, scale_sem, raw_send, raw_recv, late_sem, go,
    ) = refs[2 + len(pieces) :]
    me = lax.axis_index("shard")
    core = lax.rem(me, 2)
    items, rows, width, depth = 2 * gate.shape[0], gate.shape[1], out.shape[3], held.shape[0]
    blocks, per, half = gate.shape[2] // LANES, width // LANES, gate.shape[2] // LANES // 2
    last, chunk, wide = items - near.shape[0], rows // CHUNKS, raw.shape[1]

    def peer(d, f):
        return 2 * lax.rem(me // 2 + d, chips) + lax.rem(core + f, 2)

    def device(d, f):
        return {"shard": peer(d, f)}

    def remote(src, dst, send, recv, to):
        return pltpu.make_async_remote_copy(
            src, dst, send, recv, device_id=to, device_id_type=MESH
        )

    def await_bytes(ref, sem):
        pltpu.make_async_copy(ref, ref, sem).wait()

    def load(k):
        slot, expert = lax.rem(k, depth), k // 2

        @pl.when(lax.rem(k, 2) == 0)
        def _():
            pltpu.make_async_copy(gate.at[expert], held.at[slot], load_sem.at[slot]).start()

        @pl.when(lax.rem(k, 2) == 1)
        def _():
            pltpu.make_async_copy(up.at[expert], held.at[slot], load_sem.at[slot]).start()

    def first(c):
        at = pl.ds(c * chunk, chunk)
        return pltpu.make_async_copy(gate.at[0, at], held.at[0, at], first_sem.at[c])

    def local(k):
        slot = lax.rem(k, depth)
        await_bytes(held.at[slot], load_sem.at[slot])
        for b in range(blocks):
            values = held[slot, :, b * LANES : (b + 1) * LANES]
            mine[k, b // half, b % half : b % half + 1, :] = jnp.max(
                jnp.abs(values), axis=0, keepdims=True
            )

    def scaled(k, shard):
        slot, source = lax.rem(k, SLOTS), lax.rem(k, depth)
        for i in range(per):
            b = shard * per + i
            values = held[source, :, pl.ds(pl.multiple_of(b * LANES, LANES), LANES)]
            scale = full[k, b // half, pl.ds(lax.rem(b, half), 1), :]
            out[slot, shard, :, i * LANES : (i + 1) * LANES] = (values / scale).astype(
                jnp.bfloat16
            )

    def tell(k):
        remote(mine.at[k], beside.at[k], near_send, near_recv.at[k], device(0, 1)).start()

    def ask(k):
        await_bytes(beside.at[k], near_recv.at[k])
        whole[k] = jnp.maximum(mine[k], beside[k])
        for d in range(1, chips):
            remote(
                whole.at[k, core], cross.at[k, d - 1], cross_send, cross_recv.at[k], device(d, 0)
            ).start()

    def relay(k):
        await_bytes(cross.at[k], cross_recv.at[k])
        most = whole[k, core]
        for d in range(1, chips):
            most = jnp.maximum(most, cross[k, d - 1])
        full[k, core] = most
        remote(full.at[k, core], full.at[k, core], full_send, full_recv.at[k], device(0, 1)).start()

    def place(k, top=0):
        at = pl.ds(pl.multiple_of(me * rows + top, 16), rows - top)
        return narrow.at[lax.rem(k, 2), k // 2, at]

    def send_from(k, pieces, top):
        slot = lax.rem(k, SLOTS)
        for d, f in pieces:
            remote(
                out.at[slot, peer(d, f), pl.ds(top, rows - top)], place(k, top),
                send_sem.at[slot], recv_sem.at[jnp.minimum(k // 2, 1), 2 * d + f - 1],
                device(d, f),
            ).start()

    def send(k, pieces):
        @pl.when(k == 0)
        def _():
            send_from(0, pieces, wide)

        @pl.when(k > 0)
        def _():
            send_from(k, pieces, 0)

    def keep(k):
        slot = lax.rem(k, SLOTS)
        send_from(k, [(0, 1)], 0)
        pltpu.make_async_copy(out.at[slot, me], place(k), keep_sem.at[slot]).start()

    def first_sent():
        await_bytes(narrow.at[0, 0, pl.ds(0, (n - 1) * rows - len(away) * wide)], send_sem.at[0])
        await_bytes(out.at[0, 0], keep_sem.at[0])

    def sent(k):
        slot = lax.rem(k, SLOTS)
        await_bytes(out.at[slot, pl.ds(0, n - 1)], send_sem.at[slot])
        await_bytes(out.at[slot, 0], keep_sem.at[slot])

    def lately(j):
        d, f = away[j]
        source = peer(chips - d, f)
        to = narrow.at[0, 0, pl.ds(pl.multiple_of(source * rows, rows), wide)]
        return pltpu.make_async_copy(late.at[j], to, late_sem.at[j])

    def leave(k):
        slot, i = lax.rem(k, SLOTS), k - last
        remote(
            out.at[slot, peer(0, 1)], near.at[i, core], send_sem.at[slot], tail_recv, device(0, 1)
        ).start()
        pltpu.make_async_copy(out.at[slot, me], near.at[i, core], keep_sem.at[slot]).start()
        for (d, f, first_item, count), ref in zip(pieces, far):
            @pl.when((i >= first_item) & (i < first_item + count))
            def _():
                pltpu.make_async_copy(
                    out.at[slot, peer(d, f)], ref.at[i - first_item], keep_sem.at[slot]
                ).start()

    def left(k):
        slot = lax.rem(k, SLOTS)
        await_bytes(out.at[slot, 0], send_sem.at[slot])
        await_bytes(out.at[slot, pl.ds(0, n - 1)], keep_sem.at[slot])

    for c in range(CHUNKS):
        first(c).start()
    barrier = pltpu.get_barrier_semaphore()
    for d, f in away + [(0, 1)]:
        pl.semaphore_signal(barrier, inc=1, device_id=device(d, f), device_id_type=MESH)
    small = [
        pltpu.make_async_copy(router, weight, small_sem.at[0]),
        pltpu.make_async_copy(gain, by, small_sem.at[1]),
    ]
    for c in range(CHUNKS):
        first(c).wait()
        if c == 0:
            load(jnp.int32(1))
        for b in range(blocks):
            values = held[0, c * chunk : (c + 1) * chunk, b * LANES : (b + 1) * LANES]
            most = jnp.max(jnp.abs(values), axis=0, keepdims=True)
            at = b // half, slice(b % half, b % half + 1)
            mine[(0, *at)] = most if c == 0 else jnp.maximum(mine[(0, *at)], most)
    for k in range(2, AHEAD + 1):
        load(jnp.int32(k))
    for copy in small:
        copy.start()
    pl.semaphore_wait(barrier, n - 1)
    for j, (d, f) in enumerate(away + [(0, 1)]):
        remote(mine.at[0], direct.at[j], direct_send, direct_recv, device(d, f)).start()
    for j, (d, f) in enumerate(away):
        columns = pl.ds(pl.multiple_of(peer(d, f) * width, width), width)
        remote(
            held.at[0, pl.ds(0, wide), columns], raw.at[j], raw_send, raw_recv, device(d, f)
        ).start()
    local(1)
    load(jnp.int32(AHEAD + 1))
    tell(1)
    for copy in small:
        copy.wait()
    part[...] = (weight[...] * by[...]).astype(jnp.bfloat16)
    ask(1)
    await_bytes(direct, direct_recv)
    most = mine[0]
    for j in range(n - 1):
        most = jnp.maximum(most, direct[j])
    full[0] = most

    def step(q, _):
        @pl.when(q > 0)
        def _():
            await_bytes(full.at[q, 0], full_recv.at[q])

        @pl.when((q == SLOTS) & (core == 1))
        def _():
            first_sent()

        @pl.when(q > SLOTS)
        def _():
            sent(q - SLOTS)

        before = None
        for d, f in away + [(0, 1), (0, 0)]:
            scaled(q, peer(d, f))
            if before is not None:
                @pl.when((q < last) & (core == 0))
                def _():
                    send(q, [before])

            before = (d, f) if d > 0 else None

        @pl.when(q < last)
        def _():
            keep(q)

        @pl.when(q >= last)
        def _():
            leave(q)

        first = q + jnp.minimum(q, RAMP) + 2
        leads = [(first, first < items), (first + 1, q < RAMP)]
        for k, due in leads:
            @pl.when(due)
            def _():
                local(k)
                tell(k)

                @pl.when(k + AHEAD < items)
                def _():
                    load(k + AHEAD)

        for k, due in leads:
            @pl.when(due)
            def _():
                ask(k)

        @pl.when(q + 1 < items)
        def _():
            relay(q + 1)

        @pl.when(q == 0)
        def _():
            await_bytes(raw, raw_send)

        @pl.when((q == 1) & (core == 0))
        def _():
            first_sent()
            pl.semaphore_signal(go, inc=1, device_id=device(0, 1), device_id_type=MESH)

        @pl.when((q == 1) & (core == 1))
        def _():
            pl.semaphore_wait(go, 1)
            send(0, other)

        @pl.when((q > 0) & (q < last) & (core == 1))
        def _():
            send(q, other)

        @pl.when((q > 0) & (q <= last) & (core == 1))
        def _():
            send(q - 1, same)

        @pl.when(q == RAMP)
        def _():
            await_bytes(raw, raw_recv)
            for i in range(per):
                b = me * per + i
                scale = full[0, b // half, pl.ds(lax.rem(b, half), 1), :]
                at = slice(i * LANES, (i + 1) * LANES)
                for j in range(len(away)):
                    late[j, :, at] = (raw[j, :, at] / scale).astype(jnp.bfloat16)
            for j in range(len(away)):
                lately(j).start()
            pltpu.make_async_copy(part, pair.at[0], small_sem.at[0]).start()
            for d in range(1, chips):
                remote(part, pair.at[d], pass_send, pass_recv, device(d, 0)).start()

        return 0

    lax.fori_loop(0, items, step, 0)

    for e in range(items // 2):
        for which in (0, 1):
            for i in range(per):
                b = me * per + i
                scales[which, e : e + 1, i * LANES : (i + 1) * LANES] = full[
                    2 * e + which, b // half, pl.ds(lax.rem(b, half), 1), :
                ]

    for which, ref in enumerate((scale_gate, scale_up)):
        pltpu.make_async_copy(scales.at[which], ref, scale_sem.at[which]).start()

    def drain(k, _):
        sent(k)
        return 0

    lax.fori_loop(items - SLOTS, last, drain, 0)

    def drain_tail(k, _):
        left(k)
        return 0

    lax.fori_loop(last, items, drain_tail, 0)
    await_bytes(beside.at[pl.ds(1, items - 1)], near_send)
    await_bytes(cross.at[pl.ds(1, items - 1)], cross_send)
    await_bytes(full.at[pl.ds(1, items - 1), 0], full_send)
    await_bytes(direct, direct_send)
    rest = pair.at[pl.ds(1, chips - 1)]
    await_bytes(rest, pass_send)
    await_bytes(rest, pass_recv)
    await_bytes(part, small_sem.at[0])
    for which in (0, 1):
        await_bytes(scales.at[which], scale_sem.at[which])
    await_bytes(near.at[:, 0], tail_recv)
    for j in range(len(away)):
        lately(j).wait()
    for d, f in away + [(0, 1)]:
        j, less = 2 * d + f - 1, wide if d > 0 else 0
        await_bytes(narrow.at[0, 0, pl.ds(0, 2 * rows - less)], recv_sem.at[0, j])
        await_bytes(narrow.at[:, pl.ds(1, last // 2 - 1), pl.ds(0, rows)], recv_sem.at[1, j])


def gather(n, groups, token, pair, routers, send_sem, recv_sem, keep_sem):
    del token
    me, group, chips = lax.axis_index("shard"), lax.axis_index("expert"), n // 2
    core, (_, share, tokens) = lax.rem(me, 2), pair.shape
    column = [(f, g) for g in range(groups) for f in (0, 1) if (f, g) != (0, 0)]

    def device(f, g):
        near = me - core + lax.rem(core + f, 2)
        return {"shard": near, "expert": lax.rem(group + g, groups)}

    barrier = pltpu.get_barrier_semaphore()
    for f, g in column:
        pl.semaphore_signal(barrier, inc=1, device_id=device(f, g), device_id_type=MESH)
    pl.semaphore_wait(barrier, len(column))
    for d in range(chips):
        shard = 2 * lax.rem(me // 2 + chips - d, chips) + core
        home = routers.at[
            pl.ds(pl.multiple_of(group * share, share), share),
            pl.ds(pl.multiple_of(shard * tokens, tokens), tokens),
        ]
        for i, (f, g) in enumerate(column):
            pltpu.make_async_remote_copy(
                pair.at[d], home, send_sem.at[i], recv_sem.at[i],
                device_id=device(f, g), device_id_type=MESH,
            ).start()
        pltpu.make_async_copy(pair.at[d], home, keep_sem).start()
    for i in range(len(column)):
        pltpu.make_async_copy(pair, pair, send_sem.at[i]).wait()
        pltpu.make_async_copy(pair, pair, recv_sem.at[i]).wait()
    pltpu.make_async_copy(pair, pair, keep_sem).wait()


def spread(narrow, gate, up, token):
    gate[...] = narrow[0]
    up[...] = narrow[1]
    token[...] = jnp.zeros_like(token)


def finish(n, pieces, extras, *refs):
    count = len(pieces)
    arrived, small, results, sems = (
        refs[:count], refs[count : count + extras], refs[count + extras + 2 : -1], refs[-1]
    )
    gate, up, *copies = results
    me, chips = lax.axis_index("shard"), n // 2
    experts, rows = gate.shape[0], gate.shape[1] // n
    for at, (piece, ref) in enumerate(zip(pieces, arrived)):
        d, f, first_item, count = piece
        for i in range(count):
            item = first_item + i
            final = (gate, up)[item % 2].at[experts - TAIL + item // 2]
            for c in range(ref.shape[1]):
                if d == 0:
                    source = 2 * (me // 2) + c
                else:
                    source = 2 * lax.rem(me // 2 + chips - d, chips) + lax.rem(me % 2 + f, 2)
                to = final.at[pl.ds(pl.multiple_of(source * rows, rows), rows)]
                pltpu.make_async_copy(ref.at[i, c], to, sems.at[at]).start()
    for ref, copy in zip(small, copies):
        copy[...] = ref[...]
    for at, ref in enumerate(arrived):
        pltpu.make_async_copy(ref, ref, sems.at[at]).wait()


def by_kernel(n, groups, gate, up, router, gain):
    experts, rows, columns = gate.shape
    width, items, depth, chips = columns // n, 2 * experts, RAMP + AHEAD + 2, n // 2
    tokens, share = router.shape
    half = columns // LANES // 2
    pieces, column = tail_pieces(n), 2 * groups - 1
    f32 = functools.partial(jax.ShapeDtypeStruct, dtype=jnp.float32)
    anywhere = pl.BlockSpec(memory_space=pl.ANY)
    inside = pl.BlockSpec(memory_space=pltpu.VMEM)
    dma = pltpu.SemaphoreType.DMA
    bf16 = functools.partial(jax.ShapeDtypeStruct, dtype=jnp.bfloat16)
    maxima = pltpu.VMEM((items, 2, half, LANES), jnp.float32)
    narrow, near, *far, scale_gate, scale_up, pair = pl.pallas_call(
        functools.partial(exchange, n),
        name="exchange",
        out_shape=(
            bf16((2, experts - TAIL, n * rows, width)),
            bf16((2 * TAIL, 2, rows, width)),
            *[bf16((count, rows, width)) for *_, count in pieces],
            f32((experts, width)),
            f32((experts, width)),
            bf16((chips, share, tokens)),
        ),
        in_specs=[anywhere] * 4,
        out_specs=(anywhere,) * (5 + len(pieces)),
        scratch_shapes=[
            pltpu.VMEM((depth, rows, columns), jnp.float32),
            pltpu.VMEM((SLOTS, n, rows, width), jnp.bfloat16),
            pltpu.VMEM((share, tokens), jnp.float32),
            pltpu.VMEM((1, tokens), jnp.float32),
            pltpu.VMEM((share, tokens), jnp.bfloat16),
            pltpu.VMEM((2, experts, width), jnp.float32),
            maxima,
            maxima,
            maxima,
            pltpu.VMEM((items, chips - 1, half, LANES), jnp.float32),
            maxima,
            pltpu.VMEM((n - 1, 2, half, LANES), jnp.float32),
            pltpu.VMEM((n - 2, rows // EIGHTH, width), jnp.float32),
            pltpu.VMEM((n - 2, rows // EIGHTH, width), jnp.bfloat16),
            dma((CHUNKS,)),
            dma((depth,)),
            dma,
            dma((items,)),
            dma,
            dma((items,)),
            dma,
            dma((items,)),
            dma,
            dma,
            dma((SLOTS,)),
            dma((2, n - 1)),
            dma((SLOTS,)),
            dma,
            dma((2,)),
            dma,
            dma,
            dma((2,)),
            dma,
            dma,
            dma((n - 2,)),
            pltpu.SemaphoreType.REGULAR,
        ],
        compiler_params=pltpu.CompilerParams(collective_id=0, has_side_effects=True),
    )(gate, up, router.T, gain.reshape(1, tokens))
    arrived = []
    for (d, f, *_), ref in zip(pieces, far):
        arrived.append(lax.ppermute(ref, "shard", [(s, shift(s, d, f, chips)) for s in range(n)]))
    finals = (bf16((experts, n * rows, width)),) * 2
    *final, token = pl.pallas_call(
        spread,
        name="spread",
        grid=(experts - TAIL,),
        out_shape=finals + (f32((8, LANES)),),
        in_specs=[pl.BlockSpec((2, 1, n * rows, width), lambda e: (0, e, 0, 0))],
        out_specs=(pl.BlockSpec((1, n * rows, width), lambda e: (e, 0, 0)),) * 2
        + (pl.BlockSpec((8, LANES), lambda e: (0, 0)),),
        cost_estimate=pl.CostEstimate(flops=0, bytes_accessed=4 * narrow.size, transcendentals=0),
        compiler_params=pltpu.CompilerParams(vmem_limit_bytes=24 * 2**20),
    )(narrow)

    routers = pl.pallas_call(
        functools.partial(gather, n, groups),
        name="gather",
        out_shape=bf16((groups * share, n * tokens)),
        in_specs=[anywhere, inside],
        out_specs=anywhere,
        scratch_shapes=[dma((column,)), dma((column,)), dma],
        compiler_params=pltpu.CompilerParams(
            collective_id=1, has_side_effects=True, vmem_limit_bytes=16 * 2**20
        ),
    )(token, pair)

    def put(pieces, blocks, final, small=()):
        count = len(blocks) + len(small)
        return pl.pallas_call(
            functools.partial(finish, n, pieces, len(small)),
            out_shape=finals + tuple(jax.ShapeDtypeStruct(s.shape, s.dtype) for s in small),
            in_specs=[inside] * count + [anywhere] * 2,
            out_specs=(anywhere,) * 2 + (inside,) * len(small),
            scratch_shapes=[dma((len(blocks),))],
            input_output_aliases={count: 0, count + 1: 1},
            compiler_params=pltpu.CompilerParams(vmem_limit_bytes=16 * 2**20),
        )(*blocks, *small, *final)

    blocks = [jnp.expand_dims(ref, 1) for ref in arrived]
    third = len(pieces) // 3
    *final, scale_gate, scale_up, routers = put(
        [(0, 0, 0, 2 * TAIL)] + pieces[:third], [near] + blocks[:third], final,
        (scale_gate, scale_up, routers),
    )
    final = put(pieces[third:-third], blocks[third:-third], final)
    final_gate, final_up = put(pieces[-third:], blocks[-third:], final)
    return final_gate, final_up, scale_gate, scale_up, routers.T


def by_collectives(gate, up, router, gain):
    scale_gate, scale_up = lax.pmax(
        (jnp.max(jnp.abs(gate), axis=1), jnp.max(jnp.abs(up), axis=1)), "shard"
    )

    def serve(master, scale):
        narrow = (master / jnp.expand_dims(scale, 1)).astype(jnp.bfloat16)
        final = lax.all_to_all(narrow, "shard", split_axis=2, concat_axis=1, tiled=True)
        width = final.shape[2]
        return final, lax.dynamic_slice_in_dim(
            scale, lax.axis_index("shard") * width, width, axis=1
        )

    final_gate, scale_gate = serve(gate, scale_gate)
    final_up, scale_up = serve(up, scale_up)
    part = (router * gain[:, None]).astype(jnp.bfloat16)
    rows = lax.all_gather(part, "shard", axis=0, tiled=True)
    return final_gate, final_up, scale_gate, scale_up, lax.all_gather(rows, "expert", axis=1, tiled=True)


def solution(mesh):
    n, groups = mesh.shape["shard"], mesh.shape["expert"]

    def shards(gate, up, router, gain):
        aligned = gate.shape[2] % (n * LANES) == 0 and gate.shape[1] % (16 * CHUNKS * EIGHTH) == 0
        aligned = aligned and gate.shape[0] > TAIL + SLOTS + RAMP and 2 * TAIL <= SLOTS
        aligned = aligned and router.shape[0] % LANES == 0 and router.shape[1] % 16 == 0
        if n >= 4 and n % 2 == 0 and aligned:
            return by_kernel(n, groups, gate, up, router, gain)
        return by_collectives(gate, up, router, gain)

    return jax.shard_map(
        shards,
        mesh=mesh,
        in_specs=(
            P(("shift", "expert"), "shard", None),
            P(("shift", "expert"), "shard", None),
            P(("shift", "shard"), "expert"),
            P(("shift", "shard")),
        ),
        out_specs=(
            P(("shift", "expert"), None, "shard"),
            P(("shift", "expert"), None, "shard"),
            P(("shift", "expert"), "shard"),
            P(("shift", "expert"), "shard"),
            P("shift", None),
        ),
        check_vma=False,
    )
```

```python
import functools

import jax
import jax.numpy as jnp
from jax import lax
from jax.experimental import pallas as pl
from jax.experimental.pallas import tpu as pltpu
from jax.sharding import PartitionSpec as P


MESH = pl.DeviceIdType.MESH
LANES = 128
TAIL = 2
EARLY = 3
RAMP = 3
AHEAD = 3
SLOTS = 8
CHUNKS = 4
EIGHTH = 8


def shift(shard, d, f, chips):
    return 2 * ((shard // 2 + d) % chips) + (shard % 2 + f) % 2


def tail_pieces(n):
    ahead = range(1, n // 2)
    return (
        [(d, 0, 0, EARLY) for d in ahead]
        + [(d, 1, 0, 2 * TAIL) for d in ahead]
        + [(d, 0, EARLY, 2 * TAIL - EARLY) for d in ahead]
    )


def exchange(n, gate, up, router, gain, *refs):
    chips = n // 2
    away = [(d, f) for d in range(1, chips) for f in (0, 1)]
    same, other = [p for p in away if p[1] == 0], [p for p in away if p[1] == 1]
    pieces = tail_pieces(n)
    narrow, near, *far = refs[: 2 + len(pieces)]
    (
        scale_gate, scale_up, pair, held, out, weight, by, part, scales, mine, beside, whole, cross,
        full, direct, raw, late, first_sem, load_sem, near_send, near_recv, cross_send, cross_recv, full_send,
        full_recv, direct_send, direct_recv, send_sem, recv_sem, keep_sem, tail_recv, small_sem,
        pass_send, pass_recv, scale_sem, raw_send, raw_recv, late_sem, go,
    ) = refs[2 + len(pieces) :]
    me = lax.axis_index("shard")
    core = lax.rem(me, 2)
    items, rows, width, depth = 2 * gate.shape[0], gate.shape[1], out.shape[3], held.shape[0]
    blocks, per, half = gate.shape[2] // LANES, width // LANES, gate.shape[2] // LANES // 2
    last, chunk, wide = items - near.shape[0], rows // CHUNKS, raw.shape[1]

    def peer(d, f):
        return 2 * lax.rem(me // 2 + d, chips) + lax.rem(core + f, 2)

    def device(d, f):
        return {"shard": peer(d, f)}

    def remote(src, dst, send, recv, to):
        return pltpu.make_async_remote_copy(
            src, dst, send, recv, device_id=to, device_id_type=MESH
        )

    def await_bytes(ref, sem):
        pltpu.make_async_copy(ref, ref, sem).wait()

    def load(k):
        slot, expert = lax.rem(k, depth), k // 2

        @pl.when(lax.rem(k, 2) == 0)
        def _():
            pltpu.make_async_copy(gate.at[expert], held.at[slot], load_sem.at[slot]).start()

        @pl.when(lax.rem(k, 2) == 1)
        def _():
            pltpu.make_async_copy(up.at[expert], held.at[slot], load_sem.at[slot]).start()

    def first(c):
        at = pl.ds(c * chunk, chunk)
        return pltpu.make_async_copy(gate.at[0, at], held.at[0, at], first_sem.at[c])

    def local(k):
        slot = lax.rem(k, depth)
        await_bytes(held.at[slot], load_sem.at[slot])
        for b in range(blocks):
            values = held[slot, :, b * LANES : (b + 1) * LANES]
            mine[k, b // half, b % half : b % half + 1, :] = jnp.max(
                jnp.abs(values), axis=0, keepdims=True
            )

    def scaled(k, shard):
        slot, source = lax.rem(k, SLOTS), lax.rem(k, depth)
        for i in range(per):
            b = shard * per + i
            values = held[source, :, pl.ds(pl.multiple_of(b * LANES, LANES), LANES)]
            scale = full[k, b // half, pl.ds(lax.rem(b, half), 1), :]
            out[slot, shard, :, i * LANES : (i + 1) * LANES] = (values / scale).astype(
                jnp.bfloat16
            )

    def tell(k):
        remote(mine.at[k], beside.at[k], near_send, near_recv.at[k], device(0, 1)).start()

    def ask(k):
        await_bytes(beside.at[k], near_recv.at[k])
        whole[k] = jnp.maximum(mine[k], beside[k])
        for d in range(1, chips):
            remote(
                whole.at[k, core], cross.at[k, d - 1], cross_send, cross_recv.at[k], device(d, 0)
            ).start()

    def relay(k):
        await_bytes(cross.at[k], cross_recv.at[k])
        most = whole[k, core]
        for d in range(1, chips):
            most = jnp.maximum(most, cross[k, d - 1])
        full[k, core] = most
        remote(full.at[k, core], full.at[k, core], full_send, full_recv.at[k], device(0, 1)).start()

    def place(k, top=0):
        at = pl.ds(pl.multiple_of(me * rows + top, 16), rows - top)
        return narrow.at[lax.rem(k, 2), k // 2, at]

    def send_from(k, pieces, top):
        slot = lax.rem(k, SLOTS)
        for d, f in pieces:
            remote(
                out.at[slot, peer(d, f), pl.ds(top, rows - top)], place(k, top),
                send_sem.at[slot], recv_sem.at[jnp.minimum(k // 2, 1), 2 * d + f - 1],
                device(d, f),
            ).start()

    def send(k, pieces):
        @pl.when(k == 0)
        def _():
            send_from(0, pieces, wide)

        @pl.when(k > 0)
        def _():
            send_from(k, pieces, 0)

    def keep(k):
        slot = lax.rem(k, SLOTS)
        send_from(k, [(0, 1)], 0)
        pltpu.make_async_copy(out.at[slot, me], place(k), keep_sem.at[slot]).start()

    def first_sent():
        await_bytes(narrow.at[0, 0, pl.ds(0, (n - 1) * rows - len(away) * wide)], send_sem.at[0])
        await_bytes(out.at[0, 0], keep_sem.at[0])

    def sent(k):
        slot = lax.rem(k, SLOTS)
        await_bytes(out.at[slot, pl.ds(0, n - 1)], send_sem.at[slot])
        await_bytes(out.at[slot, 0], keep_sem.at[slot])

    def lately(j):
        d, f = away[j]
        source = peer(chips - d, f)
        to = narrow.at[0, 0, pl.ds(pl.multiple_of(source * rows, rows), wide)]
        return pltpu.make_async_copy(late.at[j], to, late_sem.at[j])

    def leave(k):
        slot, i = lax.rem(k, SLOTS), k - last
        remote(
            out.at[slot, peer(0, 1)], near.at[i, core], send_sem.at[slot], tail_recv, device(0, 1)
        ).start()
        pltpu.make_async_copy(out.at[slot, me], near.at[i, core], keep_sem.at[slot]).start()
        for (d, f, first_item, count), ref in zip(pieces, far):
            @pl.when((i >= first_item) & (i < first_item + count))
            def _():
                pltpu.make_async_copy(
                    out.at[slot, peer(d, f)], ref.at[i - first_item], keep_sem.at[slot]
                ).start()

    def left(k):
        slot = lax.rem(k, SLOTS)
        await_bytes(out.at[slot, 0], send_sem.at[slot])
        await_bytes(out.at[slot, pl.ds(0, n - 1)], keep_sem.at[slot])

    for c in range(CHUNKS):
        first(c).start()
    barrier = pltpu.get_barrier_semaphore()
    for d, f in away + [(0, 1)]:
        pl.semaphore_signal(barrier, inc=1, device_id=device(d, f), device_id_type=MESH)
    small = [
        pltpu.make_async_copy(router, weight, small_sem.at[0]),
        pltpu.make_async_copy(gain, by, small_sem.at[1]),
    ]
    for c in range(CHUNKS):
        first(c).wait()
        if c == 0:
            load(jnp.int32(1))
        for b in range(blocks):
            values = held[0, c * chunk : (c + 1) * chunk, b * LANES : (b + 1) * LANES]
            most = jnp.max(jnp.abs(values), axis=0, keepdims=True)
            at = b // half, slice(b % half, b % half + 1)
            mine[(0, *at)] = most if c == 0 else jnp.maximum(mine[(0, *at)], most)
    for k in range(2, AHEAD + 1):
        load(jnp.int32(k))
    for copy in small:
        copy.start()
    pl.semaphore_wait(barrier, n - 1)
    for j, (d, f) in enumerate(away + [(0, 1)]):
        remote(mine.at[0], direct.at[j], direct_send, direct_recv, device(d, f)).start()
    for j, (d, f) in enumerate(away):
        columns = pl.ds(pl.multiple_of(peer(d, f) * width, width), width)
        remote(
            held.at[0, pl.ds(0, wide), columns], raw.at[j], raw_send, raw_recv, device(d, f)
        ).start()
    local(1)
    load(jnp.int32(AHEAD + 1))
    tell(1)
    for copy in small:
        copy.wait()
    part[...] = (weight[...] * by[...]).astype(jnp.bfloat16)
    ask(1)
    await_bytes(direct, direct_recv)
    most = mine[0]
    for j in range(n - 1):
        most = jnp.maximum(most, direct[j])
    full[0] = most

    def step(q, _):
        @pl.when(q > 0)
        def _():
            await_bytes(full.at[q, 0], full_recv.at[q])

        @pl.when((q == SLOTS) & (core == 1))
        def _():
            first_sent()

        @pl.when(q > SLOTS)
        def _():
            sent(q - SLOTS)

        before = None
        for d, f in away + [(0, 1), (0, 0)]:
            scaled(q, peer(d, f))
            if before is not None:
                @pl.when((q < last) & (core == 0))
                def _():
                    send(q, [before])

            before = (d, f) if d > 0 else None

        @pl.when(q < last)
        def _():
            keep(q)

        @pl.when(q >= last)
        def _():
            leave(q)

        first = q + jnp.minimum(q, RAMP) + 2
        leads = [(first, first < items), (first + 1, q < RAMP)]
        for k, due in leads:
            @pl.when(due)
            def _():
                local(k)
                tell(k)

                @pl.when(k + AHEAD < items)
                def _():
                    load(k + AHEAD)

        for k, due in leads:
            @pl.when(due)
            def _():
                ask(k)

        @pl.when(q + 1 < items)
        def _():
            relay(q + 1)

        @pl.when(q == 0)
        def _():
            await_bytes(raw, raw_send)

        @pl.when((q == 1) & (core == 0))
        def _():
            first_sent()
            pl.semaphore_signal(go, inc=1, device_id=device(0, 1), device_id_type=MESH)

        @pl.when((q == 1) & (core == 1))
        def _():
            pl.semaphore_wait(go, 1)
            send(0, other)

        @pl.when((q > 0) & (q < last) & (core == 1))
        def _():
            send(q, other)

        @pl.when((q > 0) & (q <= last) & (core == 1))
        def _():
            send(q - 1, same)

        @pl.when(q == RAMP)
        def _():
            await_bytes(raw, raw_recv)
            for i in range(per):
                b = me * per + i
                scale = full[0, b // half, pl.ds(lax.rem(b, half), 1), :]
                at = slice(i * LANES, (i + 1) * LANES)
                for j in range(len(away)):
                    late[j, :, at] = (raw[j, :, at] / scale).astype(jnp.bfloat16)
            pltpu.make_async_copy(part, pair.at[0], small_sem.at[0]).start()
            for d in range(1, chips):
                remote(part, pair.at[d], pass_send, pass_recv, device(d, 0)).start()

        @pl.when(q == RAMP + 1)
        def _():
            for j in range(len(away)):
                lately(j).start()

        return 0

    lax.fori_loop(0, items, step, 0)

    for e in range(items // 2):
        for which in (0, 1):
            for i in range(per):
                b = me * per + i
                scales[which, e : e + 1, i * LANES : (i + 1) * LANES] = full[
                    2 * e + which, b // half, pl.ds(lax.rem(b, half), 1), :
                ]

    for which, ref in enumerate((scale_gate, scale_up)):
        pltpu.make_async_copy(scales.at[which], ref, scale_sem.at[which]).start()

    def drain(k, _):
        sent(k)
        return 0

    lax.fori_loop(items - SLOTS, last, drain, 0)

    def drain_tail(k, _):
        left(k)
        return 0

    lax.fori_loop(last, items, drain_tail, 0)
    await_bytes(beside.at[pl.ds(1, items - 1)], near_send)
    await_bytes(cross.at[pl.ds(1, items - 1)], cross_send)
    await_bytes(full.at[pl.ds(1, items - 1), 0], full_send)
    await_bytes(direct, direct_send)
    rest = pair.at[pl.ds(1, chips - 1)]
    await_bytes(rest, pass_send)
    await_bytes(rest, pass_recv)
    await_bytes(part, small_sem.at[0])
    for which in (0, 1):
        await_bytes(scales.at[which], scale_sem.at[which])
    await_bytes(near.at[:, 0], tail_recv)
    for j in range(len(away)):
        lately(j).wait()
    for d, f in away + [(0, 1)]:
        j, less = 2 * d + f - 1, wide if d > 0 else 0
        await_bytes(narrow.at[0, 0, pl.ds(0, 2 * rows - less)], recv_sem.at[0, j])
        await_bytes(narrow.at[:, pl.ds(1, last // 2 - 1), pl.ds(0, rows)], recv_sem.at[1, j])


def gather(n, groups, token, pair, routers, send_sem, recv_sem, keep_sem):
    del token
    me, group, chips = lax.axis_index("shard"), lax.axis_index("expert"), n // 2
    core, (_, share, tokens) = lax.rem(me, 2), pair.shape
    column = [(f, g) for g in range(groups) for f in (0, 1) if (f, g) != (0, 0)]

    def device(f, g):
        near = me - core + lax.rem(core + f, 2)
        return {"shard": near, "expert": lax.rem(group + g, groups)}

    barrier = pltpu.get_barrier_semaphore()
    for f, g in column:
        pl.semaphore_signal(barrier, inc=1, device_id=device(f, g), device_id_type=MESH)
    pl.semaphore_wait(barrier, len(column))
    for d in range(chips):
        shard = 2 * lax.rem(me // 2 + chips - d, chips) + core
        home = routers.at[
            pl.ds(pl.multiple_of(group * share, share), share),
            pl.ds(pl.multiple_of(shard * tokens, tokens), tokens),
        ]
        for i, (f, g) in enumerate(column):
            pltpu.make_async_remote_copy(
                pair.at[d], home, send_sem.at[i], recv_sem.at[i],
                device_id=device(f, g), device_id_type=MESH,
            ).start()
        pltpu.make_async_copy(pair.at[d], home, keep_sem).start()
    for i in range(len(column)):
        pltpu.make_async_copy(pair, pair, send_sem.at[i]).wait()
        pltpu.make_async_copy(pair, pair, recv_sem.at[i]).wait()
    pltpu.make_async_copy(pair, pair, keep_sem).wait()


def spread(narrow, gate, up, token):
    gate[...] = narrow[0]
    up[...] = narrow[1]
    token[...] = jnp.zeros_like(token)


def finish(n, pieces, extras, *refs):
    count = len(pieces)
    arrived, small, results, sems = (
        refs[:count], refs[count : count + extras], refs[count + extras + 2 : -1], refs[-1]
    )
    gate, up, *copies = results
    me, chips = lax.axis_index("shard"), n // 2
    experts, rows = gate.shape[0], gate.shape[1] // n
    for at, (piece, ref) in enumerate(zip(pieces, arrived)):
        d, f, first_item, count = piece
        for i in range(count):
            item = first_item + i
            final = (gate, up)[item % 2].at[experts - TAIL + item // 2]
            for c in range(ref.shape[1]):
                if d == 0:
                    source = 2 * (me // 2) + c
                else:
                    source = 2 * lax.rem(me // 2 + chips - d, chips) + lax.rem(me % 2 + f, 2)
                to = final.at[pl.ds(pl.multiple_of(source * rows, rows), rows)]
                pltpu.make_async_copy(ref.at[i, c], to, sems.at[at]).start()
    for ref, copy in zip(small, copies):
        copy[...] = ref[...]
    for at, ref in enumerate(arrived):
        pltpu.make_async_copy(ref, ref, sems.at[at]).wait()


def by_kernel(n, groups, gate, up, router, gain):
    experts, rows, columns = gate.shape
    width, items, depth, chips = columns // n, 2 * experts, RAMP + AHEAD + 2, n // 2
    tokens, share = router.shape
    half = columns // LANES // 2
    pieces, column = tail_pieces(n), 2 * groups - 1
    f32 = functools.partial(jax.ShapeDtypeStruct, dtype=jnp.float32)
    anywhere = pl.BlockSpec(memory_space=pl.ANY)
    inside = pl.BlockSpec(memory_space=pltpu.VMEM)
    dma = pltpu.SemaphoreType.DMA
    bf16 = functools.partial(jax.ShapeDtypeStruct, dtype=jnp.bfloat16)
    maxima = pltpu.VMEM((items, 2, half, LANES), jnp.float32)
    narrow, near, *far, scale_gate, scale_up, pair = pl.pallas_call(
        functools.partial(exchange, n),
        name="exchange",
        out_shape=(
            bf16((2, experts - TAIL, n * rows, width)),
            bf16((2 * TAIL, 2, rows, width)),
            *[bf16((count, rows, width)) for *_, count in pieces],
            f32((experts, width)),
            f32((experts, width)),
            bf16((chips, share, tokens)),
        ),
        in_specs=[anywhere] * 4,
        out_specs=(anywhere,) * (5 + len(pieces)),
        scratch_shapes=[
            pltpu.VMEM((depth, rows, columns), jnp.float32),
            pltpu.VMEM((SLOTS, n, rows, width), jnp.bfloat16),
            pltpu.VMEM((share, tokens), jnp.float32),
            pltpu.VMEM((1, tokens), jnp.float32),
            pltpu.VMEM((share, tokens), jnp.bfloat16),
            pltpu.VMEM((2, experts, width), jnp.float32),
            maxima,
            maxima,
            maxima,
            pltpu.VMEM((items, chips - 1, half, LANES), jnp.float32),
            maxima,
            pltpu.VMEM((n - 1, 2, half, LANES), jnp.float32),
            pltpu.VMEM((n - 2, rows // EIGHTH, width), jnp.float32),
            pltpu.VMEM((n - 2, rows // EIGHTH, width), jnp.bfloat16),
            dma((CHUNKS,)),
            dma((depth,)),
            dma,
            dma((items,)),
            dma,
            dma((items,)),
            dma,
            dma((items,)),
            dma,
            dma,
            dma((SLOTS,)),
            dma((2, n - 1)),
            dma((SLOTS,)),
            dma,
            dma((2,)),
            dma,
            dma,
            dma((2,)),
            dma,
            dma,
            dma((n - 2,)),
            pltpu.SemaphoreType.REGULAR,
        ],
        compiler_params=pltpu.CompilerParams(collective_id=0, has_side_effects=True),
    )(gate, up, router.T, gain.reshape(1, tokens))
    arrived = []
    for (d, f, *_), ref in zip(pieces, far):
        arrived.append(lax.ppermute(ref, "shard", [(s, shift(s, d, f, chips)) for s in range(n)]))
    finals = (bf16((experts, n * rows, width)),) * 2
    *final, token = pl.pallas_call(
        spread,
        name="spread",
        grid=(experts - TAIL,),
        out_shape=finals + (f32((8, LANES)),),
        in_specs=[pl.BlockSpec((2, 1, n * rows, width), lambda e: (0, e, 0, 0))],
        out_specs=(pl.BlockSpec((1, n * rows, width), lambda e: (e, 0, 0)),) * 2
        + (pl.BlockSpec((8, LANES), lambda e: (0, 0)),),
        cost_estimate=pl.CostEstimate(flops=0, bytes_accessed=4 * narrow.size, transcendentals=0),
        compiler_params=pltpu.CompilerParams(vmem_limit_bytes=24 * 2**20),
    )(narrow)

    routers = pl.pallas_call(
        functools.partial(gather, n, groups),
        name="gather",
        out_shape=bf16((groups * share, n * tokens)),
        in_specs=[anywhere, inside],
        out_specs=anywhere,
        scratch_shapes=[dma((column,)), dma((column,)), dma],
        compiler_params=pltpu.CompilerParams(
            collective_id=1, has_side_effects=True, vmem_limit_bytes=16 * 2**20
        ),
    )(token, pair)

    def put(pieces, blocks, final, small=()):
        count = len(blocks) + len(small)
        return pl.pallas_call(
            functools.partial(finish, n, pieces, len(small)),
            out_shape=finals + tuple(jax.ShapeDtypeStruct(s.shape, s.dtype) for s in small),
            in_specs=[inside] * count + [anywhere] * 2,
            out_specs=(anywhere,) * 2 + (inside,) * len(small),
            scratch_shapes=[dma((len(blocks),))],
            input_output_aliases={count: 0, count + 1: 1},
            compiler_params=pltpu.CompilerParams(vmem_limit_bytes=16 * 2**20),
        )(*blocks, *small, *final)

    blocks = [jnp.expand_dims(ref, 1) for ref in arrived]
    third = len(pieces) // 3
    *final, scale_gate, scale_up, routers = put(
        [(0, 0, 0, 2 * TAIL)] + pieces[:third], [near] + blocks[:third], final,
        (scale_gate, scale_up, routers),
    )
    final = put(pieces[third:-third], blocks[third:-third], final)
    final_gate, final_up = put(pieces[-third:], blocks[-third:], final)
    return final_gate, final_up, scale_gate, scale_up, routers.T


def by_collectives(gate, up, router, gain):
    scale_gate, scale_up = lax.pmax(
        (jnp.max(jnp.abs(gate), axis=1), jnp.max(jnp.abs(up), axis=1)), "shard"
    )

    def serve(master, scale):
        narrow = (master / jnp.expand_dims(scale, 1)).astype(jnp.bfloat16)
        final = lax.all_to_all(narrow, "shard", split_axis=2, concat_axis=1, tiled=True)
        width = final.shape[2]
        return final, lax.dynamic_slice_in_dim(
            scale, lax.axis_index("shard") * width, width, axis=1
        )

    final_gate, scale_gate = serve(gate, scale_gate)
    final_up, scale_up = serve(up, scale_up)
    part = (router * gain[:, None]).astype(jnp.bfloat16)
    rows = lax.all_gather(part, "shard", axis=0, tiled=True)
    return final_gate, final_up, scale_gate, scale_up, lax.all_gather(rows, "expert", axis=1, tiled=True)


def solution(mesh):
    n, groups = mesh.shape["shard"], mesh.shape["expert"]

    def shards(gate, up, router, gain):
        aligned = gate.shape[2] % (n * LANES) == 0 and gate.shape[1] % (16 * CHUNKS) == 0
        aligned = aligned and gate.shape[1] % (16 * EIGHTH) == 0
        aligned = aligned and gate.shape[0] > TAIL + SLOTS + RAMP and 2 * TAIL <= SLOTS
        aligned = aligned and router.shape[0] % LANES == 0 and router.shape[1] % 16 == 0
        if n >= 4 and n % 2 == 0 and aligned:
            return by_kernel(n, groups, gate, up, router, gain)
        return by_collectives(gate, up, router, gain)

    return jax.shard_map(
        shards,
        mesh=mesh,
        in_specs=(
            P(("shift", "expert"), "shard", None),
            P(("shift", "expert"), "shard", None),
            P(("shift", "shard"), "expert"),
            P(("shift", "shard")),
        ),
        out_specs=(
            P(("shift", "expert"), None, "shard"),
            P(("shift", "expert"), None, "shard"),
            P(("shift", "expert"), "shard"),
            P(("shift", "expert"), "shard"),
            P("shift", None),
        ),
        check_vma=False,
    )
```
